32 devices in a mesh: gx: 2 (over y), gy: 8 (over z, core), gz: 2 (over x).
Axes of the slice: x: 2, y: 2, z: 4, core: 2. Of those that a mesh axis runs over, the one named last changes fastest.
Arguments:
- starting_kelvin: float32 [16, 32, 2048], P(None, 'gx', ('gy', 'gz')), may hold values from -6 to 6
- substance_label: int32 [16, 32, 2048], P(None, 'gx', ('gy', 'gz')), may hold values from 0 to 3
- voxel_source_patch: int32 [16, 32, 2048], P(None, 'gx', ('gy', 'gz')), may hold values from 0 to 15
- substance_traits: float32 [4, 4], replicated, may hold values from 0.5 to 2
- patch_source_intensity: float32 [16], replicated, may hold values from 0 to 8
Outputs:
- warmed_result: float32 [16, 32, 2048], P(None, 'gx', ('gy', 'gz'))
- solution: float32 [3, 16, 32, 2048], P(None, 'gz', 'gx', 'gy')
- residual: float32 [3, 16, 32, 2048], P(None, 'gz', 'gx', 'gy')
The draws below stay inside these ranges and needn't reach their ends.
All inputs are finite; a program needn't handle non-finite values.
Results may differ from the reference program's by a relative error of at most 0.0029.
Values sent between devices are 32-bit elements; how exact they have to be, the bound alone decides.
A program may use at most 64 MiB of HBM per device.

```python
import math
import jax
import jax.numpy as jnp

HEIGHT_VOXELS = 16
MATS = 4
TILES = 16
HEAT_STEPS = 2
ITERS = 3
LATERAL_DEPTH = 32
LATERAL_WIDTH = 2048


def with_ends(entries, own_key, low, high):
    longest = entries.shape.index(max(entries.shape))
    spots = []
    for shift in (0, 1):
        where = [jax.random.randint(jax.random.fold_in(own_key, axis), (), 0, length) for axis, length in enumerate(entries.shape)]
        where[longest] = (where[longest] + shift) % entries.shape[longest]
        spots.append(tuple(where))
    return entries.at[spots[0]].set(low).at[spots[1]].set(high)


def shard_levels(key, shape, shards, least, top_value):
    def one(dim, shards_of):
        steps = jax.random.uniform(jax.random.fold_in(jax.random.fold_in(key, 6), dim), (shards_of,), jnp.float32, least / len(shards), top_value / len(shards))
        return jnp.repeat(jnp.exp(steps), shape[dim] // shards_of).reshape((-1,) + (1,) * (len(shape) - dim - 1))

    gain = one(*shards[0])
    for cut in shards[1:]:
        gain = gain * one(*cut)
    return gain


def scatter_about(stream_key, extent, spread, limit, cuts=(), held_as=jnp.bfloat16):
    entries = spread * jax.random.normal(stream_key, extent, jnp.float32)
    if cuts:
        entries = entries * shard_levels(stream_key, extent, cuts, -0.22, 0.18)
    return jnp.clip(entries, -limit, limit).astype(held_as)


def setup_inputs(seed: int = 0) -> dict:
    arg_keys = jax.random.split(jax.random.key(seed), 6)
    return {
        "starting_kelvin": scatter_about(arg_keys[0], (HEIGHT_VOXELS, LATERAL_DEPTH, LATERAL_WIDTH), 1.0, 6.0, ((1, 2), (2, 16)), jnp.float32),
        "substance_label": with_ends(jax.random.randint(arg_keys[1], (HEIGHT_VOXELS, LATERAL_DEPTH, LATERAL_WIDTH), 0, MATS), jax.random.fold_in(arg_keys[1], 1), 0, MATS - 1).astype(jnp.int32),
        "voxel_source_patch": with_ends(jax.random.randint(arg_keys[2], (HEIGHT_VOXELS, LATERAL_DEPTH, LATERAL_WIDTH), 0, TILES), jax.random.fold_in(arg_keys[2], 1), 0, TILES - 1).astype(jnp.int32),
        "substance_traits": jnp.clip(jnp.exp(jax.random.uniform(arg_keys[3], (4, MATS), jnp.float32, math.log(0.5), math.log(2.0))), 0.5, 2.0),
        "patch_source_intensity": jnp.clip(jax.random.uniform(arg_keys[4], (TILES,), jnp.float32, 0.0, 8.0), 0.0, 8.0),
    }


time_step = 0.03
anchor_scale = 0.5
strain_gain = 2.0


def lookup(identity, table, count):
    summed = jnp.zeros(identity.shape, jnp.float32)
    for number in range(count):
        summed = summed + jnp.where(identity == number, table[number], jnp.float32(0.0))
    return summed


def conduct(own, other):
    return 2.0 * own * other / jnp.maximum(own + other, 0.25)


def heat_step(padded_temp, padded_cond, power, inverse_cap):
    centre = padded_temp[:, 1:-1, 1:-1]
    own = padded_cond[:, 1:-1, 1:-1]
    layers, rows, columns = centre.shape
    heat_flux = jnp.zeros_like(centre)
    for row_offset, column_offset in ((0, 1), (2, 1), (1, 0), (1, 2)):
        neighbour = padded_temp[:, row_offset:row_offset + rows, column_offset:column_offset + columns]
        other = padded_cond[:, row_offset:row_offset + rows, column_offset:column_offset + columns]
        heat_flux = heat_flux + conduct(own, other) * (neighbour - centre)
    vertical_temp = jnp.pad(centre, ((1, 1), (0, 0), (0, 0)))
    vertical_cond = jnp.pad(own, ((1, 1), (0, 0), (0, 0)))
    for layer_offset in (0, 2):
        other = vertical_cond[layer_offset:layer_offset + layers]
        neighbour = vertical_temp[layer_offset:layer_offset + layers]
        heat_flux = heat_flux + conduct(own, other) * (neighbour - centre)
    return centre + time_step * inverse_cap * (heat_flux + power)


def neighbour_offsets():
    listed = []
    for along_z in (-1, 0, 1):
        for along_x in (-1, 0, 1):
            for along_y in (-1, 0, 1):
                if along_z != 0 or along_x != 0 or along_y != 0:
                    listed.append((along_z, along_x, along_y))
    return listed


def apply_operator(field, padded_field, modulus, padded_modulus):
    layers, rows, columns = modulus.shape
    parts = [anchor_scale * modulus * field[0], anchor_scale * modulus * field[1], anchor_scale * modulus * field[2]]
    for along_z, along_x, along_y in neighbour_offsets():
        length_sq = along_z * along_z + along_x * along_x + along_y * along_y
        window = (slice(1 + along_z, 1 + along_z + layers), slice(1 + along_x, 1 + along_x + rows), slice(1 + along_y, 1 + along_y + columns))
        weight = (0.5 / length_sq) * (modulus + padded_modulus[window])
        change = [field[index_c] - padded_field[index_c][window] for index_c in range(3)]
        projected = (along_z * change[0] + along_x * change[1] + along_y * change[2]) / length_sq
        for index_c, direction_part in enumerate((along_z, along_x, along_y)):
            parts[index_c] = parts[index_c] + weight * (0.5 * change[index_c] + direction_part * projected)
    return jnp.stack(parts)


def thermal_load(modulus, padded_modulus, strain, padded_strain):
    layers, rows, columns = modulus.shape
    parts = [jnp.zeros_like(modulus), jnp.zeros_like(modulus), jnp.zeros_like(modulus)]
    for along_z, along_x, along_y in neighbour_offsets():
        length_sq = along_z * along_z + along_x * along_x + along_y * along_y
        window = (slice(1 + along_z, 1 + along_z + layers), slice(1 + along_x, 1 + along_x + rows), slice(1 + along_y, 1 + along_y + columns))
        weight = (0.5 / length_sq) * (modulus + padded_modulus[window])
        pushing = weight * (0.5 * (strain + padded_strain[window]))
        for index_c, direction_part in enumerate((along_z, along_x, along_y)):
            if direction_part != 0:
                parts[index_c] = parts[index_c] - strain_gain * direction_part * pushing
    return jnp.stack(parts)


def reference(starting_kelvin, substance_label, voxel_source_patch, substance_traits, patch_source_intensity):
    diffusive_coefficient = lookup(substance_label, substance_traits[0], MATS)
    inverse_cap = 1.0 / lookup(substance_label, substance_traits[1], MATS)
    power = lookup(voxel_source_patch, patch_source_intensity, TILES)
    cycle = ((0, 0), (1, 1), (1, 1))
    padded_cond = jnp.pad(diffusive_coefficient, cycle)
    warmed_result = starting_kelvin
    for number in range(HEAT_STEPS):
        warmed_result = heat_step(jnp.pad(warmed_result, cycle), padded_cond, power, inverse_cap)
    modulus = lookup(substance_label, substance_traits[2], MATS)
    strain = lookup(substance_label, substance_traits[3], MATS) * warmed_result
    padded_modulus = jnp.pad(modulus, 1)
    load = thermal_load(modulus, padded_modulus, strain, jnp.pad(strain, 1))
    solution = jnp.zeros_like(load)
    residual = load
    direction = load
    norm_now = jnp.sum(residual * residual)
    shell = ((0, 0), (1, 1), (1, 1), (1, 1))
    for number in range(ITERS):
        image = apply_operator(direction, jnp.pad(direction, shell), modulus, padded_modulus)
        alpha = norm_now / jnp.sum(direction * image)
        solution = solution + alpha * direction
        residual = residual - alpha * image
        norm_next = jnp.sum(residual * residual)
        direction = residual + (norm_next / norm_now) * direction
        norm_now = norm_next
    return warmed_result, solution, residual
```

```python
import functools

import jax
import jax.numpy as jnp
from jax import lax
from jax.experimental import pallas as pl
from jax.experimental.pallas import tpu as pltpu
from jax.sharding import PartitionSpec as P

ITERS = 3
HALO = 8
TIME_STEP = 0.03
ANCHOR = 0.5
K_TOTAL = 4 * 0.25 + 4 * 0.125 + 2 * (0.75 + 4 * 0.25 + 4 * 5.0 / 36.0)
MESH = pl.DeviceIdType.MESH
DIRECTIONS = [(dx, dc) for dx in (-1, 0, 1) for dc in (-1, 0, 1) if (dx, dc) != (0, 0)]


def shift(f, axis, step):
    return pltpu.roll(f, (-step) % f.shape[axis], axis)


def sums(f, axis):
    after, before = shift(f, axis, 1), shift(f, axis, -1)
    return after + before, after - before


def matrix_parts(f):
    sy, dy = sums(f, 1)
    sx, dx = sums(f, 0)
    sxsy, dxsy = sums(sy, 0)
    sxdy, dxdy = sums(dy, 0)
    return sx, sy, sxsy, dx * 0.125 + dxsy * (1.0 / 18.0), dy * 0.125 + sxdy * (1.0 / 18.0), dxdy


def diag_z(f, sx, sy, sxsy):
    near = 0.25 * (sx + sy)
    return near + 0.125 * sxsy, 0.75 * f + near + (5.0 / 36.0) * sxsy


def diag_x(f, sx, sy, sxsy):
    near = 0.25 * sy
    return 0.75 * sx + near + 0.25 * sxsy, 0.25 * (f + sx) + 0.125 * sy + (5.0 / 36.0) * sxsy


def diag_y(f, sx, sy, sxsy):
    near = 0.25 * sx
    return 0.75 * sy + near + 0.25 * sxsy, 0.25 * (f + sy) + 0.125 * sx + (5.0 / 36.0) * sxsy


def vector_stencil(uz, ux, uy):
    sx, sy, sxsy, ex, ey, _ = matrix_parts(uz)
    z0, z1 = diag_z(uz, sx, sy, sxsy)
    dif_x, dif_y = ex, ey
    sx, sy, sxsy, ex, _, cross_x = matrix_parts(ux)
    x0, x1 = diag_x(ux, sx, sy, sxsy)
    dif_z = ex
    sx, sy, sxsy, _, ey, cross_y = matrix_parts(uy)
    y0, y1 = diag_y(uy, sx, sy, sxsy)
    dif_z = dif_z + ey
    x0, x1 = x0 + 0.125 * cross_y, x1 + (1.0 / 18.0) * cross_y
    y0, y1 = y0 + 0.125 * cross_x, y1 + (1.0 / 18.0) * cross_x
    return (z0, x0, y0), (z1, x1, y1), (dif_z, dif_x, dif_y)


def gradient_stencil(f):
    sy, dy = sums(f, 1)
    sx, dx = sums(f, 0)
    sxsy, dxsy = sums(sy, 0)
    sxdy, _ = sums(dy, 0)
    zero = jnp.zeros_like(f)
    return (
        (zero, 0.5 * dx + 0.25 * dxsy, 0.5 * dy + 0.25 * sxdy),
        (zero, 0.25 * dx + (1.0 / 6.0) * dxsy, 0.25 * dy + (1.0 / 6.0) * sxdy),
        (0.5 * f + 0.25 * (sx + sy) + (1.0 / 6.0) * sxsy, zero, zero),
    )


def stream(layers, count, zero, planes, emit, extra):
    def body(p, carry):
        held, below, extra = carry
        same, both, diff = planes(p)
        out = [h + b + d for h, b, d in zip(held, both, diff)]
        extra = emit(p - 1, out, extra)
        held = [w + s for w, s in zip(below, same)]
        below = [b - d for b, d in zip(both, diff)]
        return held, below, extra

    zeros = [zero] * count
    return lax.fori_loop(1, layers + 2, body, (zeros, list(zeros), extra))[2]


def kernel(
    sizes,
    kelvin, label, patch, traits, power_table,
    warmed, solution, residual,
    temp, temp2, lab, pat, cond, mod, strain, mask, gx_s, gy_s, gz_s, rate_s, pow_s, mats,
    v, vrecv, pack_f, pack_i, got_f, got_i, red_src, red_buf,
    local_sem, send_sem, recv_sem, vsend_sem, vrecv_sem, rsend_sem, rrecv_sem,
):
    nx, ny, nz = sizes
    nc, total = ny * nz, nx * ny * nz
    layers, rows, cols = kelvin.shape
    share = layers // nz
    full_rows = rows + 2 * HALO
    shape = (full_rows, 2 * cols)
    ix, iy, iz = lax.axis_index("gx"), lax.axis_index("gy"), lax.axis_index("gz")
    ic = iy * nz + iz
    me = ix * nc + ic

    def coords(flat):
        return (flat // nc, (flat % nc) // nz, flat % nz)

    barrier = pltpu.get_barrier_semaphore()

    def greet(k, _):
        pl.semaphore_signal(
            barrier, inc=1, device_id=coords(lax.rem(me + k, total)), device_id_type=MESH
        )
        return 0

    lax.fori_loop(1, total, greet, 0)

    own = (slice(None), pl.ds(HALO, rows), pl.ds(0, cols))
    local = [
        pltpu.make_async_copy(a, b.at[own], local_sem.at[i])
        for i, (a, b) in enumerate(((kelvin, temp), (label, lab), (patch, pat)))
    ]
    for copy in local:
        copy.start()

    lane = lax.broadcasted_iota(jnp.int32, (rows, cols), 1)
    sources = (kelvin, label, patch)
    for side in (0, 1):
        for index, ref in enumerate(sources):
            packed = jnp.zeros((rows, cols), ref.dtype)
            for z in range(layers):
                amount = (HALO * z + (HALO if side else 0)) % cols
                piece = ref[z]
                piece = pltpu.roll(piece, amount, 1) if amount else piece
                packed = jnp.where(lane // HALO == z, piece, packed)
            if index == 0:
                pack_f[side] = packed
            else:
                pack_i[side, index - 1] = packed

    pl.semaphore_wait(barrier, total - 1)

    def transfers(number):
        dx, dc = DIRECTIONS[number]
        there = (lax.rem(ix + dx + nx, nx) * nc) + lax.rem(ic + dc + nc, nc)
        target = jnp.logical_and(
            jnp.logical_and(ix + dx >= 0, ix + dx < nx), jnp.logical_and(ic + dc >= 0, ic + dc < nc)
        )
        origin = jnp.logical_and(
            jnp.logical_and(ix - dx >= 0, ix - dx < nx), jnp.logical_and(ic - dc >= 0, ic - dc < nc)
        )
        if dx == 0:
            from_rows, to_rows = pl.ds(0, rows), pl.ds(HALO, rows)
        elif dx == 1:
            from_rows, to_rows = pl.ds(rows - HALO, HALO), pl.ds(0, HALO)
        else:
            from_rows, to_rows = pl.ds(0, HALO), pl.ds(HALO + rows, HALO)
        if dc == 0:
            pairs = [
                (ref.at[:, from_rows, :], ext.at[:, to_rows, pl.ds(0, cols)])
                for ref, ext in zip(sources, (temp, lab, pat))
            ]
        else:
            side = (dc + 1) // 2
            pairs = [(pack_f.at[side, from_rows, :], got_f.at[side, to_rows, :])]
            pairs += [
                (pack_i.at[side, i, from_rows, :], got_i.at[side, i, to_rows, :]) for i in (0, 1)
            ]
        copies = [
            pltpu.make_async_remote_copy(
                src_ref=a, dst_ref=b, send_sem=send_sem.at[number, i],
                recv_sem=recv_sem.at[number, i], device_id=coords(there), device_id_type=MESH,
            )
            for i, (a, b) in enumerate(pairs)
        ]
        return target, origin, copies, to_rows, dc

    moves = [transfers(i) for i in range(len(DIRECTIONS))]
    for target, _, copies, _, _ in moves:
        @pl.when(target)
        def _(copies=copies):
            for copy in copies:
                copy.start()

    for _, origin, _, to_rows, dc in moves:
        @pl.when(jnp.logical_not(origin))
        def _(to_rows=to_rows, dc=dc):
            if dc == 0:
                block = (layers, to_rows.size, cols)
                temp[:, to_rows, 0:cols] = jnp.zeros(block, jnp.float32)
                lab[:, to_rows, 0:cols] = jnp.full(block, -1, jnp.int32)
                pat[:, to_rows, 0:cols] = jnp.zeros(block, jnp.int32)
            else:
                side = (dc + 1) // 2
                block = (to_rows.size, cols)
                got_f[side, to_rows, :] = jnp.zeros(block, jnp.float32)
                got_i[side, 0, to_rows, :] = jnp.full(block, -1, jnp.int32)
                got_i[side, 1, to_rows, :] = jnp.zeros(block, jnp.int32)

    empty = jnp.zeros(shape, jnp.float32)
    for end in (0, layers + 1):
        for ref in (mod, strain, mask):
            ref[end] = empty
        for k in range(ITERS):
            for c in range(3):
                v[k, c, end] = empty
    for c in range(6):
        mats[c, 0] = empty
    cond[layers] = empty

    shift_scalar = 3.0 * (traits[2, 0] + traits[2, 1] + traits[2, 2] + traits[2, 3])
    inverse_shift = 1.0 / jnp.full((1, 2 * cols), shift_scalar, jnp.float32)

    for copy in local:
        copy.wait()
    for _, origin, copies, _, _ in moves:
        @pl.when(origin)
        def _(copies=copies):
            for copy in copies:
                copy.wait_recv()

    halo_lane = lax.broadcasted_iota(jnp.int32, (full_rows, cols), 1)
    materials = traits.shape[1]
    tiles = power_table.shape[0]

    def prepare(z, _):
        def unpack(left, right, outside):
            left = pltpu.roll(left, lax.rem(2 * cols - HALO - HALO * z, cols), 1)
            right = pltpu.roll(right, lax.rem(cols - HALO * z, cols), 1)
            rest = jnp.where(halo_lane >= cols - HALO, left, outside)
            return jnp.where(halo_lane < HALO, right, rest)

        temp[z, :, cols:] = unpack(got_f[1], got_f[0], jnp.float32(0.0))
        label_halo = unpack(got_i[1, 0], got_i[0, 0], jnp.int32(-1))
        patch_halo = unpack(got_i[1, 1], got_i[0, 1], jnp.int32(0))
        for part, ids, patches in (
            (pl.ds(0, cols), lab[z, :, 0:cols], pat[z, :, 0:cols]),
            (pl.ds(cols, cols), label_halo, patch_halo),
        ):
            values = [jnp.zeros(ids.shape, jnp.float32) for _ in range(4)]
            for m in range(materials):
                hit = ids == m
                values = [jnp.where(hit, traits[q, m], values[q]) for q in range(4)]
            inside = ids >= 0
            cond[z, :, part] = values[0]
            rate_s[z, :, part] = jnp.where(inside, TIME_STEP / jnp.where(inside, values[1], 1.0), 0.0)
            mod[z + 1, :, part] = values[2] * inverse_shift[:, 0:cols]
            strain[z + 1, :, part] = values[3]
            mask[z + 1, :, part] = jnp.where(inside, 1.0, 0.0)
            power = jnp.zeros(ids.shape, jnp.float32)
            for t in range(tiles):
                power = jnp.where(patches == t, power_table[t], power)
            pow_s[z, :, part] = power
        return 0

    lax.fori_loop(0, layers, prepare, 0)

    def conduct(a, b):
        return 2.0 * a * b / jnp.maximum(a + b, 0.25)

    def heat(z, flow_below, source, first):
        centre = source[z]
        if first:
            own_cond = cond[z]
            along_x = conduct(own_cond, shift(own_cond, 0, 1))
            along_y = conduct(own_cond, shift(own_cond, 1, 1))
            along_z = conduct(own_cond, cond[z + 1])
            gx_s[z], gy_s[z], gz_s[z] = along_x, along_y, along_z
        else:
            along_x, along_y, along_z = gx_s[z], gy_s[z], gz_s[z]
        flow_x = along_x * (shift(centre, 0, 1) - centre)
        flow_y = along_y * (shift(centre, 1, 1) - centre)
        flow_z = along_z * (source[jnp.minimum(z + 1, layers - 1)] - centre)
        flux = flow_x - shift(flow_x, 0, -1) + flow_y - shift(flow_y, 1, -1) + flow_z - flow_below
        return centre + rate_s[z] * (flux + pow_s[z]), flow_z

    def first_step(z, flow_below):
        temp2[z], flow_z = heat(z, flow_below, temp, True)
        return flow_z

    blank = mod[0]
    lax.fori_loop(0, layers, first_step, blank)

    def second_step(z, flow_below):
        value, flow_z = heat(z, flow_below, temp2, False)
        warmed[z] = value[HALO : HALO + rows, 0:cols]
        strain[z + 1] = strain[z + 1] * value
        return flow_z

    lax.fori_loop(0, layers, second_step, blank)

    def matrix_planes(p):
        f = mod[p]
        sx, sy, sxsy, ex, ey, cross = matrix_parts(f)
        z0, z1 = diag_z(f, sx, sy, sxsy)
        x0, x1 = diag_x(f, sx, sy, sxsy)
        y0, y1 = diag_y(f, sx, sy, sxsy)
        zero = jnp.zeros_like(f)
        return (
            (z0, x0, y0, zero, zero, 0.125 * cross),
            (z1, x1, y1, zero, zero, (1.0 / 18.0) * cross),
            (zero, zero, zero, ex, ey, zero),
        )

    def matrix_emit(p, out, extra):
        diagonal = (ANCHOR + K_TOTAL) * mod[p] - 1.0
        for c in range(6):
            mats[c, p] = out[c] + diagonal if c < 3 else out[c]
        return extra

    stream(layers, 6, blank, matrix_planes, matrix_emit, 0)

    def fold(value):
        inner = value[HALO : HALO + rows, 0:cols]
        result = inner[0:8]
        for r in range(8, rows, 8):
            result = result + inner[r : r + 8]
        return result

    tile = mod[0, 0:8, 0:cols]

    def load_planes(p):
        m, s = mod[p], strain[p]
        parts = [gradient_stencil(f) for f in (s, m, m * s)]
        return tuple(tuple(a for part in parts for a in part[i]) for i in range(3))

    def load_emit(p, out, acc):
        m, s, inside = mod[p], strain[p], mask[p]
        for c in range(3):
            value = -inside * (m * out[c] + s * out[3 + c] + out[6 + c])
            v[0, c, p] = value
            acc = acc + fold(value * value)
        return acc

    moments = [stream(layers, 9, blank, load_planes, load_emit, tile)]

    def shares(k):
        found = []
        for step in range(1, nz):
            there = lax.rem(iz + step, nz)
            found.append(
                pltpu.make_async_remote_copy(
                    src_ref=v.at[k, :, pl.ds(1 + there * share, share), pl.ds(HALO, rows), pl.ds(0, cols)],
                    dst_ref=vrecv.at[k, step - 1],
                    send_sem=vsend_sem.at[k, step - 1], recv_sem=vrecv_sem.at[k, step - 1],
                    device_id=(ix, iy, there), device_id_type=MESH,
                )
            )
        return found

    sharing = [shares(k) for k in range(ITERS + 1)]
    for copy in sharing[0]:
        copy.start()

    for k in range(ITERS):
        def planes(p, k=k):
            m = mod[p]
            u = [v[k, c, p] for c in range(3)]
            first = vector_stencil(*u)
            second = vector_stencil(*[m * f for f in u])
            return tuple(a + b for a, b in zip(first, second))

        def emit(p, out, acc, k=k):
            m, inside = mod[p], mask[p]
            u = [v[k, c, p] for c in range(3)]
            zz, xx, yy, zx, zy, xy = [mats[c, p] for c in range(6)]
            grown = (
                zz * u[0] + zx * u[1] + zy * u[2],
                zx * u[0] + xx * u[1] + xy * u[2],
                zy * u[0] + xy * u[1] + yy * u[2],
            )
            odd, even = acc
            for c in range(3):
                value = inside * (grown[c] - m * out[c] - out[3 + c])
                v[k + 1, c, p] = value
                odd = odd + fold(value * u[c])
                even = even + fold(value * value)
            return odd, even

        odd, even = stream(layers, 6, blank, planes, emit, (tile, tile))
        moments += [odd, even]
        for copy in sharing[k + 1]:
            copy.start()

    moments = moments[: 2 * ITERS]
    lane8 = lax.broadcasted_iota(jnp.int32, (1, cols), 1)
    row = jnp.zeros((1, cols), jnp.float32)
    for k, value in enumerate(moments):
        line = jnp.sum(value, axis=0, keepdims=True)
        row = jnp.where(lane8 == k, jnp.sum(line, axis=1, keepdims=True), row)
    red_src[...] = row
    red_buf[me] = row

    def spread(k):
        there = lax.rem(me + k, total)
        return pltpu.make_async_remote_copy(
            src_ref=red_src, dst_ref=red_buf.at[me], send_sem=rsend_sem.at[k],
            recv_sem=rrecv_sem.at[k], device_id=coords(there), device_id_type=MESH,
        )

    def collect(k):
        there = lax.rem(me + total - k, total)
        return pltpu.make_async_remote_copy(
            src_ref=red_src, dst_ref=red_buf.at[there], send_sem=rsend_sem.at[k],
            recv_sem=rrecv_sem.at[k], device_id=coords(there), device_id_type=MESH,
        )

    def start(k, _):
        spread(k).start()
        return 0

    def finish(k, _):
        collect(k).wait_recv()
        return 0

    def sent(k, _):
        spread(k).wait_send()
        return 0

    lax.fori_loop(1, total, start, 0)
    lax.fori_loop(1, total, finish, 0)

    def add(k, acc):
        return acc + red_buf[k]

    summed = lax.fori_loop(0, total, add, jnp.zeros((1, cols), jnp.float32))
    m = [
        jnp.sum(jnp.where(lane8 == k, summed, 0.0), axis=1, keepdims=True) for k in range(2 * ITERS)
    ]

    def inner(a, b):
        value = None
        for i, x in enumerate(a):
            for j, y in enumerate(b):
                if x is not None and y is not None:
                    term = x * y * m[i + j]
                    value = term if value is None else value + term
        return value

    def plus(a, factor, b):
        out = []
        for x, y in zip(a, b):
            if y is None:
                out.append(x)
            else:
                out.append(factor * y if x is None else x + factor * y)
        return out

    one = jnp.ones((1, 1), jnp.float32)
    size = ITERS + 1
    res = [one] + [None] * ITERS
    dire = list(res)
    sol = [None] * size
    rr = m[0]
    for number in range(ITERS):
        image = plus(list(dire), 1.0, [None] + dire[:-1])
        alpha = rr / inner(dire, image)
        sol = plus(sol, alpha, dire)
        res = plus(res, -alpha, image)
        if number + 1 < ITERS:
            new = inner(res, res)
            dire = plus(res, new / rr, dire)
            rr = new
    res = [shift_scalar * x for x in res]

    for k in range(ITERS + 1):
        for copy in sharing[k]:
            copy.wait_recv()

    for step in range(nz):
        where = pl.ds(pl.multiple_of(lax.rem(iz + nz - step, nz) * cols, cols), cols)

        def combine(z, _, step=step, where=where):
            for c in range(3):
                if step == 0:
                    parts = [
                        v[k, c, 1 + iz * share + z, pl.ds(HALO, rows), pl.ds(0, cols)]
                        for k in range(size)
                    ]
                else:
                    parts = [vrecv[k, step - 1, c, z] for k in range(size)]
                total_s = sol[0] * parts[0]
                total_r = res[0] * parts[0]
                for k in range(1, size):
                    if sol[k] is not None:
                        total_s = total_s + sol[k] * parts[k]
                    total_r = total_r + res[k] * parts[k]
                solution[c, z, :, where] = total_s
                residual[c, z, :, where] = total_r
            return 0

        lax.fori_loop(0, share, combine, 0)

    for target, _, copies, _, _ in moves:
        @pl.when(target)
        def _(copies=copies):
            for copy in copies:
                copy.wait_send()
    for k in range(ITERS + 1):
        for copy in sharing[k]:
            copy.wait_send()
    lax.fori_loop(1, total, sent, 0)


def per_device(sizes, *arrays):
    nx, ny, nz = sizes
    layers, rows, cols = arrays[0].shape
    total = nx * ny * nz
    share = layers // nz
    ext = (rows + 2 * HALO, 2 * cols)
    f32, i32 = jnp.float32, jnp.int32
    vmem = pltpu.VMEM
    dma = pltpu.SemaphoreType.DMA
    out = jax.ShapeDtypeStruct((3, share, rows, cols * nz), f32)
    plane = vmem((layers, *ext), f32)
    padded = vmem((layers + 2, *ext), f32)
    return pl.pallas_call(
        functools.partial(kernel, sizes),
        out_shape=(jax.ShapeDtypeStruct((layers, rows, cols), f32), out, out),
        in_specs=[pl.BlockSpec(memory_space=pltpu.VMEM)] * 3
        + [pl.BlockSpec(memory_space=pltpu.SMEM)] * 2,
        out_specs=[pl.BlockSpec(memory_space=pltpu.VMEM)] * 3,
        scratch_shapes=[
            plane, plane, vmem((layers, *ext), i32), vmem((layers, *ext), i32),
            vmem((layers + 1, *ext), f32), padded, padded, padded,
            plane, plane, plane, plane, plane,
            vmem((6, layers + 1, *ext), f32),
            vmem((ITERS + 1, 3, layers + 2, *ext), f32),
            vmem((ITERS + 1, nz - 1, 3, share, rows, cols), f32),
            vmem((2, rows, cols), f32), vmem((2, 2, rows, cols), i32),
            vmem((2, ext[0], cols), f32), vmem((2, 2, ext[0], cols), i32),
            vmem((1, cols), f32), vmem((total, 1, cols), f32),
            dma((3,)), dma((8, 3)), dma((8, 3)),
            dma((ITERS + 1, nz - 1)), dma((ITERS + 1, nz - 1)), dma((total,)), dma((total,)),
        ],
        compiler_params=pltpu.CompilerParams(
            collective_id=0, has_side_effects=True, vmem_limit_bytes=60 * 1024 * 1024
        ),
    )(*arrays)


def solution(mesh):
    sizes = tuple(mesh.shape[axis] for axis in ("gx", "gy", "gz"))
    split = P(None, "gx", ("gy", "gz"))
    out = P(None, "gz", "gx", "gy")
    return jax.shard_map(
        functools.partial(per_device, sizes),
        mesh=mesh,
        in_specs=(split, split, split, P(), P()),
        out_specs=(split, out, out),
        check_vma=False,
    )
```

```python
import functools

import jax
import jax.numpy as jnp
from jax import lax
from jax.experimental import pallas as pl
from jax.experimental.pallas import tpu as pltpu
from jax.sharding import PartitionSpec as P

ITERS = 3
HALO = 8
EDGE = 4
TIME_STEP = 0.03
ANCHOR = 0.5
K_TOTAL = 4 * 0.25 + 4 * 0.125 + 2 * (0.75 + 4 * 0.25 + 4 * 5.0 / 36.0)
MESH = pl.DeviceIdType.MESH
DIRECTIONS = [(dx, dc) for dx in (-1, 0, 1) for dc in (-1, 0, 1) if (dx, dc) != (0, 0)]


def shift(f, axis, step):
    return pltpu.roll(f, (-step) % f.shape[axis], axis)


def sums(f, axis):
    after, before = shift(f, axis, 1), shift(f, axis, -1)
    return after + before, after - before


def matrix_parts(f, width=None):
    sy, dy = sums(f, 1)
    if width is not None:
        f, sy, dy = f[:, :width], sy[:, :width], dy[:, :width]
    sx, dx = sums(f, 0)
    sxsy, dxsy = sums(sy, 0)
    sxdy, dxdy = sums(dy, 0)
    return sx, sy, sxsy, dx * 0.125 + dxsy * (1.0 / 18.0), dy * 0.125 + sxdy * (1.0 / 18.0), dxdy


def diag_z(f, sx, sy, sxsy):
    near = 0.25 * (sx + sy)
    return near + 0.125 * sxsy, 0.75 * f + near + (5.0 / 36.0) * sxsy


def diag_x(f, sx, sy, sxsy):
    near = 0.25 * sy
    return 0.75 * sx + near + 0.25 * sxsy, 0.25 * (f + sx) + 0.125 * sy + (5.0 / 36.0) * sxsy


def diag_y(f, sx, sy, sxsy):
    near = 0.25 * sx
    return 0.75 * sy + near + 0.25 * sxsy, 0.25 * (f + sy) + 0.125 * sx + (5.0 / 36.0) * sxsy


def vector_stencil(uz, ux, uy, width):
    sx, sy, sxsy, ex, ey, _ = matrix_parts(uz, width)
    uz, ux_in, uy_in = uz[:, :width], ux[:, :width], uy[:, :width]
    z0, z1 = diag_z(uz, sx, sy, sxsy)
    dif_x, dif_y = ex, ey
    sx, sy, sxsy, ex, _, cross_x = matrix_parts(ux, width)
    x0, x1 = diag_x(ux_in, sx, sy, sxsy)
    dif_z = ex
    sx, sy, sxsy, _, ey, cross_y = matrix_parts(uy, width)
    y0, y1 = diag_y(uy_in, sx, sy, sxsy)
    dif_z = dif_z + ey
    x0, x1 = x0 + 0.125 * cross_y, x1 + (1.0 / 18.0) * cross_y
    y0, y1 = y0 + 0.125 * cross_x, y1 + (1.0 / 18.0) * cross_x
    return (z0, x0, y0), (z1, x1, y1), (dif_z, dif_x, dif_y)


def gradient_stencil(f):
    sy, dy = sums(f, 1)
    sx, dx = sums(f, 0)
    sxsy, dxsy = sums(sy, 0)
    sxdy, _ = sums(dy, 0)
    zero = jnp.zeros_like(f)
    return (
        (zero, 0.5 * dx + 0.25 * dxsy, 0.5 * dy + 0.25 * sxdy),
        (zero, 0.25 * dx + (1.0 / 6.0) * dxsy, 0.25 * dy + (1.0 / 6.0) * sxdy),
        (0.5 * f + 0.25 * (sx + sy) + (1.0 / 6.0) * sxsy, zero, zero),
    )


def stream(layers, count, zero, planes, emit, extra):
    def body(p, carry):
        held, below, extra = carry
        same, both, diff = planes(p)
        out = [h + b + d for h, b, d in zip(held, both, diff)]
        extra = emit(p - 1, out, extra)
        held = [w + s for w, s in zip(below, same)]
        below = [b - d for b, d in zip(both, diff)]
        return held, below, extra

    zeros = [zero] * count
    return lax.fori_loop(1, layers + 2, body, (zeros, list(zeros), extra))[2]


def kernel(
    sizes,
    kelvin, label, patch, traits, power_table,
    warmed_out, solution_out, residual_out,
    warmed, solution, residual, vown, moment_s, out_sem,
    temp, temp2, lab, pat, cond, mod, strain, mask, gx_s, gy_s, gz_s, rate_s, pow_s, mats,
    v, vrecv, pack_f, pack_i, got_f, got_i, red_src, red_buf,
    local_sem, send_sem, recv_sem, vsend_sem, vrecv_sem, rsend_sem, rrecv_sem,
):
    nx, ny, nz = sizes
    nc, total = ny * nz, nx * ny * nz
    layers, rows, cols = kelvin.shape
    share = layers // nz
    full_rows = rows + 2 * HALO
    shape = (full_rows, 2 * cols)
    kept = slice(HALO - EDGE, HALO + rows + EDGE)
    inner_rows = slice(EDGE, EDGE + rows)
    ix, iy, iz = lax.axis_index("gx"), lax.axis_index("gy"), lax.axis_index("gz")
    ic = iy * nz + iz
    me = ix * nc + ic

    def coords(flat):
        return (flat // nc, (flat % nc) // nz, flat % nz)

    barrier = pltpu.get_barrier_semaphore()

    def greet(k, _):
        pl.semaphore_signal(
            barrier, inc=1, device_id=coords(lax.rem(me + k, total)), device_id_type=MESH
        )
        return 0

    lax.fori_loop(1, total, greet, 0)

    own = (slice(None), pl.ds(HALO, rows), pl.ds(0, cols))
    local = [
        pltpu.make_async_copy(a, b.at[own], local_sem.at[i])
        for i, (a, b) in enumerate(((kelvin, temp), (label, lab), (patch, pat)))
    ]
    for copy in local:
        copy.start()

    lane = lax.broadcasted_iota(jnp.int32, (rows, cols), 1)
    sources = (kelvin, label, patch)
    for copy in local:
        copy.wait()
    for side in (0, 1):
        for index, ref in enumerate((temp, lab, pat)):
            packed = jnp.zeros((rows, cols), ref.dtype)
            for z in range(layers):
                amount = (HALO * z + (HALO if side else 0)) % cols
                piece = ref[(z, *own[1:])]
                piece = pltpu.roll(piece, amount, 1) if amount else piece
                packed = jnp.where(lane // HALO == z, piece, packed)
            if index == 0:
                pack_f[side] = packed
            else:
                pack_i[side, index - 1] = packed

    pl.semaphore_wait(barrier, total - 1)

    def transfers(number):
        dx, dc = DIRECTIONS[number]
        there = (lax.rem(ix + dx + nx, nx) * nc) + lax.rem(ic + dc + nc, nc)
        target = jnp.logical_and(
            jnp.logical_and(ix + dx >= 0, ix + dx < nx), jnp.logical_and(ic + dc >= 0, ic + dc < nc)
        )
        origin = jnp.logical_and(
            jnp.logical_and(ix - dx >= 0, ix - dx < nx), jnp.logical_and(ic - dc >= 0, ic - dc < nc)
        )
        if dx == 0:
            from_rows, to_rows = pl.ds(0, rows), pl.ds(HALO, rows)
        elif dx == 1:
            from_rows, to_rows = pl.ds(rows - HALO, HALO), pl.ds(0, HALO)
        else:
            from_rows, to_rows = pl.ds(0, HALO), pl.ds(HALO + rows, HALO)
        if dc == 0:
            pairs = [
                (ref.at[:, from_rows, :], ext.at[:, to_rows, pl.ds(0, cols)])
                for ref, ext in zip(sources, (temp, lab, pat))
            ]
        else:
            side = (dc + 1) // 2
            pairs = [(pack_f.at[side, from_rows, :], got_f.at[side, to_rows, :])]
            pairs += [
                (pack_i.at[side, i, from_rows, :], got_i.at[side, i, to_rows, :]) for i in (0, 1)
            ]
        copies = [
            pltpu.make_async_remote_copy(
                src_ref=a, dst_ref=b, send_sem=send_sem.at[number, i],
                recv_sem=recv_sem.at[number, i], device_id=coords(there), device_id_type=MESH,
            )
            for i, (a, b) in enumerate(pairs)
        ]
        return target, origin, copies, to_rows, dc

    moves = [transfers(i) for i in range(len(DIRECTIONS))]
    for target, _, copies, _, _ in moves:
        @pl.when(target)
        def _(copies=copies):
            for copy in copies:
                copy.start()

    for _, origin, _, to_rows, dc in moves:
        @pl.when(jnp.logical_not(origin))
        def _(to_rows=to_rows, dc=dc):
            if dc == 0:
                block = (layers, to_rows.size, cols)
                temp[:, to_rows, 0:cols] = jnp.zeros(block, jnp.float32)
                lab[:, to_rows, 0:cols] = jnp.full(block, -1, jnp.int32)
                pat[:, to_rows, 0:cols] = jnp.zeros(block, jnp.int32)
            else:
                side = (dc + 1) // 2
                block = (to_rows.size, cols)
                got_f[side, to_rows, :] = jnp.zeros(block, jnp.float32)
                got_i[side, 0, to_rows, :] = jnp.full(block, -1, jnp.int32)
                got_i[side, 1, to_rows, :] = jnp.zeros(block, jnp.int32)

    empty = jnp.zeros(shape, jnp.float32)
    blank_kept = jnp.zeros((rows + 2 * EDGE, 2 * cols), jnp.float32)
    for end in (0, layers + 1):
        for ref in (mod, strain, mask):
            ref[end] = blank_kept
        for k in range(ITERS):
            for c in range(3):
                v[k, c, end] = blank_kept
    for c in range(6):
        mats[c, 0] = blank_kept
    cond[layers] = empty

    shift_scalar = 3.0 * (traits[2, 0] + traits[2, 1] + traits[2, 2] + traits[2, 3])
    inverse_shift = 1.0 / jnp.full((1, 2 * cols), shift_scalar, jnp.float32)

    for _, origin, copies, _, _ in moves:
        @pl.when(origin)
        def _(copies=copies):
            for copy in copies:
                copy.wait_recv()

    halo_lane = lax.broadcasted_iota(jnp.int32, (full_rows, cols), 1)
    materials = traits.shape[1]
    tiles = power_table.shape[0]

    def prepare(z, _):
        def unpack(left, right, outside):
            left = pltpu.roll(left, lax.rem(2 * cols - HALO - HALO * z, cols), 1)
            right = pltpu.roll(right, lax.rem(cols - HALO * z, cols), 1)
            rest = jnp.where(halo_lane >= cols - HALO, left, outside)
            return jnp.where(halo_lane < HALO, right, rest)

        temp[z, :, cols:] = unpack(got_f[1], got_f[0], jnp.float32(0.0))
        label_halo = unpack(got_i[1, 0], got_i[0, 0], jnp.int32(-1))
        patch_halo = unpack(got_i[1, 1], got_i[0, 1], jnp.int32(0))
        for part, ids, patches in (
            (pl.ds(0, cols), lab[z, :, 0:cols], pat[z, :, 0:cols]),
            (pl.ds(cols, cols), label_halo, patch_halo),
        ):
            near = ids[kept]
            values = [jnp.zeros(a.shape, jnp.float32) for a in (ids, ids, near, near)]
            for m in range(materials):
                hit, near_hit = ids == m, near == m
                hits = (hit, hit, near_hit, near_hit)
                values = [jnp.where(hits[q], traits[q, m], values[q]) for q in range(4)]
            inside = ids >= 0
            cond[z, :, part] = values[0]
            rate_s[z, :, part] = jnp.where(inside, TIME_STEP / jnp.where(inside, values[1], 1.0), 0.0)
            mod[z + 1, :, part] = values[2] * inverse_shift[:, 0:cols]
            strain[z + 1, :, part] = values[3]
            mask[z + 1, :, part] = jnp.where(near >= 0, 1.0, 0.0)
            power = jnp.zeros(ids.shape, jnp.float32)
            for t in range(tiles):
                power = jnp.where(patches == t, power_table[t], power)
            pow_s[z, :, part] = power
        return 0

    lax.fori_loop(0, layers, prepare, 0)

    def conduct(a, b):
        return 2.0 * a * b / jnp.maximum(a + b, 0.25)

    def heat(z, flow_below, source, first):
        centre = source[z]
        if first:
            own_cond = cond[z]
            along_x = conduct(own_cond, shift(own_cond, 0, 1))
            along_y = conduct(own_cond, shift(own_cond, 1, 1))
            along_z = conduct(own_cond, cond[z + 1])
            gx_s[z], gy_s[z], gz_s[z] = along_x, along_y, along_z
        else:
            along_x, along_y, along_z = gx_s[z], gy_s[z], gz_s[z]
        flow_x = along_x * (shift(centre, 0, 1) - centre)
        flow_y = along_y * (shift(centre, 1, 1) - centre)
        flow_z = along_z * (source[jnp.minimum(z + 1, layers - 1)] - centre)
        flux = flow_x - shift(flow_x, 0, -1) + flow_y - shift(flow_y, 1, -1) + flow_z - flow_below
        return centre + rate_s[z] * (flux + pow_s[z]), flow_z

    def first_step(z, flow_below):
        temp2[z], flow_z = heat(z, flow_below, temp, True)
        return flow_z

    blank = mod[0]
    lax.fori_loop(0, layers, first_step, cond[layers])

    def second_step(z, flow_below):
        value, flow_z = heat(z, flow_below, temp2, False)
        warmed[z] = value[HALO : HALO + rows, 0:cols]
        strain[z + 1] = strain[z + 1] * value[kept]
        return flow_z

    lax.fori_loop(0, layers, second_step, cond[layers])
    results = [pltpu.make_async_copy(warmed, warmed_out, out_sem.at[0])]
    results[0].start()


    def matrix_planes(p):
        f = mod[p]
        sx, sy, sxsy, ex, ey, cross = matrix_parts(f)
        z0, z1 = diag_z(f, sx, sy, sxsy)
        x0, x1 = diag_x(f, sx, sy, sxsy)
        y0, y1 = diag_y(f, sx, sy, sxsy)
        zero = jnp.zeros_like(f)
        return (
            (z0, x0, y0, zero, zero, 0.125 * cross),
            (z1, x1, y1, zero, zero, (1.0 / 18.0) * cross),
            (zero, zero, zero, ex, ey, zero),
        )

    def matrix_emit(p, out, extra):
        diagonal = (ANCHOR + K_TOTAL) * mod[p] - 1.0
        for c in range(6):
            mats[c, p] = out[c] + diagonal if c < 3 else out[c]
        return extra

    stream(layers, 6, blank, matrix_planes, matrix_emit, 0)

    def fold(inner):
        result = inner[0:8]
        for r in range(8, rows, 8):
            result = result + inner[r : r + 8]
        return result

    tile = mod[0, 0:8, 0:cols]

    def load_planes(p):
        m, s = mod[p], strain[p]
        parts = [gradient_stencil(f) for f in (s, m, m * s)]
        return tuple(tuple(a for part in parts for a in part[i]) for i in range(3))

    def load_emit(p, out, acc):
        m, s, inside = mod[p], strain[p], mask[p]
        for c in range(3):
            value = -inside * (m * out[c] + s * out[3 + c] + out[6 + c])
            v[0, c, p] = value
            inner = value[inner_rows, 0:cols]
            vown[0, c, p] = inner
            acc = acc + fold(inner * inner)
        return acc

    moment_s[0] = stream(layers, 9, blank, load_planes, load_emit, tile)

    def shares(k):
        found = []
        for step in range(1, nz):
            there = lax.rem(iz + step, nz)
            found.append(
                pltpu.make_async_remote_copy(
                    src_ref=vown.at[k, :, pl.ds(1 + there * share, share)],
                    dst_ref=vrecv.at[k, step - 1],
                    send_sem=vsend_sem.at[k, step - 1], recv_sem=vrecv_sem.at[k, step - 1],
                    device_id=(ix, iy, there), device_id_type=MESH,
                )
            )
        return found

    def share_basis(k):
        for copy in shares(k):
            copy.start()

    share_basis(0)

    def apply(k, width):
        def planes(p):
            m = mod[p]
            u = [v[k, c, p] for c in range(3)]
            first = vector_stencil(*u, width)
            second = vector_stencil(*[m * f for f in u], width)
            return tuple(a + b for a, b in zip(first, second))

        def emit(p, out, acc):
            m = mod[p, :, 0:width]
            u = [v[k, c, p, :, 0:width] for c in range(3)]
            zz, xx, yy, zx, zy, xy = [mats[c, p, :, 0:width] for c in range(6)]
            grown = (
                zz * u[0] + zx * u[1] + zy * u[2],
                zx * u[0] + xx * u[1] + xy * u[2],
                zy * u[0] + xy * u[1] + yy * u[2],
            )
            odd, even = acc
            for c in range(3):
                value = grown[c] - m * out[c] - out[3 + c]
                if width > cols:
                    value = mask[p] * value
                    v[k + 1, c, p] = value
                inner = value[inner_rows, 0:cols]
                vown[k + 1, c, p] = inner
                odd = odd + fold(inner * vown[k, c, p])
                even = even + fold(inner * inner)
            return odd, even

        odd, even = stream(layers, 6, mod[0, :, 0:width], planes, emit, (tile, tile))
        moment_s[2 * k + 1] = odd
        moment_s[2 * k + 2] = even

    def grow(k, _):
        apply(k, 2 * cols)
        share_basis(k + 1)
        return 0

    lax.fori_loop(0, ITERS - 1, grow, 0)
    apply(ITERS - 1, cols)

    lane8 = lax.broadcasted_iota(jnp.int32, (1, cols), 1)
    row = jnp.zeros((1, cols), jnp.float32)
    for k in range(2 * ITERS):
        line = jnp.sum(moment_s[k], axis=0, keepdims=True)
        row = jnp.where(lane8 == k, jnp.sum(line, axis=1, keepdims=True), row)
    red_src[...] = row
    red_buf[me] = row

    def spread(k):
        there = lax.rem(me + k, total)
        return pltpu.make_async_remote_copy(
            src_ref=red_src, dst_ref=red_buf.at[me], send_sem=rsend_sem.at[k],
            recv_sem=rrecv_sem.at[k], device_id=coords(there), device_id_type=MESH,
        )

    def collect(k):
        there = lax.rem(me + total - k, total)
        return pltpu.make_async_remote_copy(
            src_ref=red_src, dst_ref=red_buf.at[there], send_sem=rsend_sem.at[k],
            recv_sem=rrecv_sem.at[k], device_id=coords(there), device_id_type=MESH,
        )

    def start(k, _):
        spread(k).start()
        return 0

    def finish(k, _):
        collect(k).wait_recv()
        return 0

    def sent(k, _):
        spread(k).wait_send()
        return 0

    lax.fori_loop(1, total, start, 0)
    share_basis(ITERS)
    lax.fori_loop(1, total, finish, 0)

    def add(k, acc):
        return acc + red_buf[k]

    summed = lax.fori_loop(0, total, add, jnp.zeros((1, cols), jnp.float32))
    m = [
        jnp.sum(jnp.where(lane8 == k, summed, 0.0), axis=1, keepdims=True) for k in range(2 * ITERS)
    ]

    def inner(a, b):
        value = None
        for i, x in enumerate(a):
            for j, y in enumerate(b):
                if x is not None and y is not None:
                    term = x * y * m[i + j]
                    value = term if value is None else value + term
        return value

    def plus(a, factor, b):
        out = []
        for x, y in zip(a, b):
            if y is None:
                out.append(x)
            else:
                out.append(factor * y if x is None else x + factor * y)
        return out

    one = jnp.ones((1, 1), jnp.float32)
    size = ITERS + 1
    res = [one] + [None] * ITERS
    dire = list(res)
    sol = [None] * size
    rr = m[0]
    for number in range(ITERS):
        image = plus(list(dire), 1.0, [None] + dire[:-1])
        alpha = rr / inner(dire, image)
        sol = plus(sol, alpha, dire)
        res = plus(res, -alpha, image)
        if number + 1 < ITERS:
            new = inner(res, res)
            dire = plus(res, new / rr, dire)
            rr = new
    res = [shift_scalar * x for x in res]

    for step in range(nz):
        where = pl.ds(pl.multiple_of(lax.rem(iz + nz - step, nz) * cols, cols), cols)
        if step:
            for k in range(size):
                shares(k)[step - 1].wait_recv()

        def combine(z, _, step=step, where=where):
            for c in range(3):
                if step == 0:
                    parts = [vown[k, c, 1 + iz * share + z] for k in range(size)]
                else:
                    parts = [vrecv[k, step - 1, c, z] for k in range(size)]
                total_s = sol[0] * parts[0]
                total_r = res[0] * parts[0]
                for k in range(1, size):
                    if sol[k] is not None:
                        total_s = total_s + sol[k] * parts[k]
                    total_r = total_r + res[k] * parts[k]
                solution[step, c, z] = total_s
                residual[step, c, z] = total_r
            return 0

        lax.fori_loop(0, share, combine, 0)
        for index, (a, b) in enumerate(((solution, solution_out), (residual, residual_out))):
            results.append(
                pltpu.make_async_copy(
                    a.at[step], b.at[:, :, :, where], out_sem.at[1 + 2 * step + index]
                )
            )
            results[-1].start()

    for target, _, copies, _, _ in moves:
        @pl.when(target)
        def _(copies=copies):
            for copy in copies:
                copy.wait_send()
    for k in range(ITERS + 1):
        for copy in shares(k):
            copy.wait_send()
    lax.fori_loop(1, total, sent, 0)
    for copy in results:
        copy.wait()


def per_device(sizes, *arrays):
    nx, ny, nz = sizes
    layers, rows, cols = arrays[0].shape
    total = nx * ny * nz
    share = layers // nz
    ext = (rows + 2 * HALO, 2 * cols)
    f32, i32 = jnp.float32, jnp.int32
    vmem = pltpu.VMEM
    dma = pltpu.SemaphoreType.DMA
    out = jax.ShapeDtypeStruct((3, share, rows, cols * nz), f32)
    plane = vmem((layers, *ext), f32)
    kept = (rows + 2 * EDGE, 2 * cols)
    padded = vmem((layers + 2, *kept), f32)
    half = vmem((nz, 3, share, rows, cols), f32)
    return pl.pallas_call(
        functools.partial(kernel, sizes),
        out_shape=(jax.ShapeDtypeStruct((layers, rows, cols), f32), out, out),
        in_specs=[pl.BlockSpec(memory_space=pl.ANY)] * 3
        + [pl.BlockSpec(memory_space=pltpu.SMEM)] * 2,
        out_specs=[pl.BlockSpec(memory_space=pl.ANY)] * 3,
        scratch_shapes=[
            vmem((layers, rows, cols), f32), half, half,
            vmem((ITERS + 1, 3, layers + 1, rows, cols), f32),
            vmem((2 * ITERS + 1, 8, cols), f32), dma((1 + 2 * nz,)),
            plane, plane, vmem((layers, *ext), i32), vmem((layers, *ext), i32),
            vmem((layers + 1, *ext), f32), padded, padded, padded,
            plane, plane, plane, plane, plane,
            vmem((6, layers + 1, *kept), f32),
            vmem((ITERS, 3, layers + 2, *kept), f32),
            vmem((ITERS + 1, nz - 1, 3, share, rows, cols), f32),
            vmem((2, rows, cols), f32), vmem((2, 2, rows, cols), i32),
            vmem((2, ext[0], cols), f32), vmem((2, 2, ext[0], cols), i32),
            vmem((1, cols), f32), vmem((total, 1, cols), f32),
            dma((3,)), dma((8, 3)), dma((8, 3)),
            dma((ITERS + 1, nz - 1)), dma((ITERS + 1, nz - 1)), dma((total,)), dma((total,)),
        ],
        compiler_params=pltpu.CompilerParams(
            collective_id=0, has_side_effects=True, vmem_limit_bytes=40 * 1024 * 1024
        ),
    )(*arrays)


def solution(mesh):
    sizes = tuple(mesh.shape[axis] for axis in ("gx", "gy", "gz"))
    split = P(None, "gx", ("gy", "gz"))
    out = P(None, "gz", "gx", "gy")
    return jax.shard_map(
        functools.partial(per_device, sizes),
        mesh=mesh,
        in_specs=(split, split, split, P(), P()),
        out_specs=(split, out, out),
        check_vma=False,
    )
```

```python
import functools

import jax
import jax.numpy as jnp
from jax import lax
from jax.experimental import pallas as pl
from jax.experimental.pallas import tpu as pltpu
from jax.sharding import PartitionSpec as P

ITERS = 3
HALO = 8
EDGE = 4
TIME_STEP = 0.03
ANCHOR = 0.5
K_TOTAL = 4 * 0.25 + 4 * 0.125 + 2 * (0.75 + 4 * 0.25 + 4 * 5.0 / 36.0)
MESH = pl.DeviceIdType.MESH
DIRECTIONS = [(dx, dc) for dx in (-1, 0, 1) for dc in (-1, 0, 1) if (dx, dc) != (0, 0)]


def shift(f, axis, step):
    return pltpu.roll(f, (-step) % f.shape[axis], axis)


def sums(f, axis):
    after, before = shift(f, axis, 1), shift(f, axis, -1)
    return after + before, after - before


def matrix_parts(f, width=None):
    sy, dy = sums(f, 1)
    if width is not None:
        f, sy, dy = f[:, :width], sy[:, :width], dy[:, :width]
    sx, dx = sums(f, 0)
    sxsy, dxsy = sums(sy, 0)
    sxdy, dxdy = sums(dy, 0)
    return sx, sy, sxsy, dx * 0.125 + dxsy * (1.0 / 18.0), dy * 0.125 + sxdy * (1.0 / 18.0), dxdy


def diag_z(f, sx, sy, sxsy):
    near = 0.25 * (sx + sy)
    return near + 0.125 * sxsy, 0.75 * f + near + (5.0 / 36.0) * sxsy


def diag_x(f, sx, sy, sxsy):
    near = 0.25 * sy
    return 0.75 * sx + near + 0.25 * sxsy, 0.25 * (f + sx) + 0.125 * sy + (5.0 / 36.0) * sxsy


def diag_y(f, sx, sy, sxsy):
    near = 0.25 * sx
    return 0.75 * sy + near + 0.25 * sxsy, 0.25 * (f + sy) + 0.125 * sx + (5.0 / 36.0) * sxsy


def vector_stencil(uz, ux, uy, width):
    sx, sy, sxsy, ex, ey, _ = matrix_parts(uz, width)
    uz, ux_in, uy_in = uz[:, :width], ux[:, :width], uy[:, :width]
    z0, z1 = diag_z(uz, sx, sy, sxsy)
    dif_x, dif_y = ex, ey
    sx, sy, sxsy, ex, _, cross_x = matrix_parts(ux, width)
    x0, x1 = diag_x(ux_in, sx, sy, sxsy)
    dif_z = ex
    sx, sy, sxsy, _, ey, cross_y = matrix_parts(uy, width)
    y0, y1 = diag_y(uy_in, sx, sy, sxsy)
    dif_z = dif_z + ey
    x0, x1 = x0 + 0.125 * cross_y, x1 + (1.0 / 18.0) * cross_y
    y0, y1 = y0 + 0.125 * cross_x, y1 + (1.0 / 18.0) * cross_x
    return (z0, x0, y0), (z1, x1, y1), (dif_z, dif_x, dif_y)


def gradient_stencil(f):
    sy, dy = sums(f, 1)
    sx, dx = sums(f, 0)
    sxsy, dxsy = sums(sy, 0)
    sxdy, _ = sums(dy, 0)
    zero = jnp.zeros_like(f)
    return (
        (zero, 0.5 * dx + 0.25 * dxsy, 0.5 * dy + 0.25 * sxdy),
        (zero, 0.25 * dx + (1.0 / 6.0) * dxsy, 0.25 * dy + (1.0 / 6.0) * sxdy),
        (0.5 * f + 0.25 * (sx + sy) + (1.0 / 6.0) * sxsy, zero, zero),
    )


def stream(layers, count, zero, planes, emit, extra):
    def body(p, carry):
        held, below, extra = carry
        same, both, diff = planes(p)
        out = [h + b + d for h, b, d in zip(held, both, diff)]
        extra = emit(p - 1, out, extra)
        held = [w + s for w, s in zip(below, same)]
        below = [b - d for b, d in zip(both, diff)]
        return held, below, extra

    zeros = [zero] * count
    return lax.fori_loop(1, layers + 2, body, (zeros, list(zeros), extra))[2]


def kernel(
    sizes,
    kelvin, label, patch, traits_in, power_in,
    warmed_out, solution_out, residual_out,
    traits, power_table, table_sem, warmed, solution, residual, vown, moment_s, out_sem,
    temp, temp2, lab, pat, cond, mod, strain, mask, gx_s, gy_s, gz_s, rate_s, pow_s, mats,
    v, vrecv, pack_f, pack_i, got_f, got_i, red_src, red_buf,
    local_sem, send_sem, recv_sem, vsend_sem, vrecv_sem, rsend_sem, rrecv_sem,
):
    nx, ny, nz = sizes
    nc, total = ny * nz, nx * ny * nz
    layers, rows, cols = kelvin.shape
    share = layers // nz
    full_rows = rows + 2 * HALO
    shape = (full_rows, 2 * cols)
    kept = slice(HALO - EDGE, HALO + rows + EDGE)
    inner_rows = slice(EDGE, EDGE + rows)
    ix, iy, iz = lax.axis_index("gx"), lax.axis_index("gy"), lax.axis_index("gz")
    ic = iy * nz + iz
    me = ix * nc + ic

    def coords(flat):
        return (flat // nc, (flat % nc) // nz, flat % nz)

    barrier = pltpu.get_barrier_semaphore()

    def greet(k, _):
        pl.semaphore_signal(
            barrier, inc=1, device_id=coords(lax.rem(me + k, total)), device_id_type=MESH
        )
        return 0

    lax.fori_loop(1, total, greet, 0)

    own = (slice(None), pl.ds(HALO, rows), pl.ds(0, cols))
    local = [
        pltpu.make_async_copy(a, b.at[own], local_sem.at[i])
        for i, (a, b) in enumerate(((kelvin, temp), (label, lab), (patch, pat)))
    ]
    tables = [
        pltpu.make_async_copy(traits_in, traits, table_sem.at[0]),
        pltpu.make_async_copy(power_in, power_table, table_sem.at[1]),
    ]
    for copy in local + tables:
        copy.start()

    sources = (kelvin, label, patch)
    pl.semaphore_wait(barrier, total - 1)

    def transfers(number):
        dx, dc = DIRECTIONS[number]
        there = (lax.rem(ix + dx + nx, nx) * nc) + lax.rem(ic + dc + nc, nc)
        target = jnp.logical_and(
            jnp.logical_and(ix + dx >= 0, ix + dx < nx), jnp.logical_and(ic + dc >= 0, ic + dc < nc)
        )
        origin = jnp.logical_and(
            jnp.logical_and(ix - dx >= 0, ix - dx < nx), jnp.logical_and(ic - dc >= 0, ic - dc < nc)
        )
        if dx == 0:
            from_rows, to_rows = pl.ds(0, rows), pl.ds(HALO, rows)
        elif dx == 1:
            from_rows, to_rows = pl.ds(rows - HALO, HALO), pl.ds(0, HALO)
        else:
            from_rows, to_rows = pl.ds(0, HALO), pl.ds(HALO + rows, HALO)
        if dc == 0:
            pairs = [
                (ref.at[:, from_rows, :], ext.at[:, to_rows, pl.ds(0, cols)])
                for ref, ext in zip(sources, (temp, lab, pat))
            ]
        else:
            side = (dc + 1) // 2
            pairs = [(pack_f.at[side, from_rows, :], got_f.at[side, to_rows, :])]
            pairs += [
                (pack_i.at[side, i, from_rows, :], got_i.at[side, i, to_rows, :]) for i in (0, 1)
            ]
        copies = [
            pltpu.make_async_remote_copy(
                src_ref=a, dst_ref=b, send_sem=send_sem.at[number, i],
                recv_sem=recv_sem.at[number, i], device_id=coords(there), device_id_type=MESH,
            )
            for i, (a, b) in enumerate(pairs)
        ]
        return target, origin, copies, to_rows, dc

    moves = [transfers(i) for i in range(len(DIRECTIONS))]
    for target, _, copies, _, dc in moves:
        if dc != 0:
            continue

        @pl.when(target)
        def _(copies=copies):
            for copy in copies:
                copy.start()

    lane = lax.broadcasted_iota(jnp.int32, (rows, cols), 1)
    for copy in local:
        copy.wait()
    for side in (0, 1):
        for index, ref in enumerate((temp, lab, pat)):
            packed = jnp.zeros((rows, cols), ref.dtype)
            for z in range(layers):
                amount = (HALO * z + (HALO if side else 0)) % cols
                piece = ref[(z, *own[1:])]
                piece = pltpu.roll(piece, amount, 1) if amount else piece
                packed = jnp.where(lane // HALO == z, piece, packed)
            if index == 0:
                pack_f[side] = packed
            else:
                pack_i[side, index - 1] = packed

    for target, _, copies, _, dc in moves:
        if dc == 0:
            continue

        @pl.when(target)
        def _(copies=copies):
            for copy in copies:
                copy.start()

    for _, origin, _, to_rows, dc in moves:
        @pl.when(jnp.logical_not(origin))
        def _(to_rows=to_rows, dc=dc):
            if dc == 0:
                block = (layers, to_rows.size, cols)
                temp[:, to_rows, 0:cols] = jnp.zeros(block, jnp.float32)
                lab[:, to_rows, 0:cols] = jnp.full(block, -1, jnp.int32)
                pat[:, to_rows, 0:cols] = jnp.zeros(block, jnp.int32)
            else:
                side = (dc + 1) // 2
                block = (to_rows.size, cols)
                got_f[side, to_rows, :] = jnp.zeros(block, jnp.float32)
                got_i[side, 0, to_rows, :] = jnp.full(block, -1, jnp.int32)
                got_i[side, 1, to_rows, :] = jnp.zeros(block, jnp.int32)

    empty = jnp.zeros(shape, jnp.float32)
    blank_kept = jnp.zeros((rows + 2 * EDGE, 2 * cols), jnp.float32)
    for end in (0, layers + 1):
        for ref in (mod, strain, mask):
            ref[end] = blank_kept
        for k in range(ITERS):
            for c in range(3):
                v[k, c, end] = blank_kept
    for c in range(6):
        mats[c, 0] = blank_kept
    cond[layers] = empty

    for copy in tables:
        copy.wait()
    shift_scalar = 3.0 * (traits[2, 0] + traits[2, 1] + traits[2, 2] + traits[2, 3])
    inverse_shift = 1.0 / jnp.full((1, 2 * cols), shift_scalar, jnp.float32)

    for _, origin, copies, _, _ in moves:
        @pl.when(origin)
        def _(copies=copies):
            for copy in copies:
                copy.wait_recv()

    halo_lane = lax.broadcasted_iota(jnp.int32, (full_rows, cols), 1)
    materials = traits.shape[1]
    tiles = power_table.shape[0]

    def prepare(z, _):
        def unpack(left, right, outside):
            left = pltpu.roll(left, lax.rem(2 * cols - HALO - HALO * z, cols), 1)
            right = pltpu.roll(right, lax.rem(cols - HALO * z, cols), 1)
            rest = jnp.where(halo_lane >= cols - HALO, left, outside)
            return jnp.where(halo_lane < HALO, right, rest)

        temp[z, :, cols:] = unpack(got_f[1], got_f[0], jnp.float32(0.0))
        label_halo = unpack(got_i[1, 0], got_i[0, 0], jnp.int32(-1))
        patch_halo = unpack(got_i[1, 1], got_i[0, 1], jnp.int32(0))
        for part, ids, patches in (
            (pl.ds(0, cols), lab[z, :, 0:cols], pat[z, :, 0:cols]),
            (pl.ds(cols, cols), label_halo, patch_halo),
        ):
            near = ids[kept]
            values = [jnp.zeros(a.shape, jnp.float32) for a in (ids, ids, near, near)]
            for m in range(materials):
                hit, near_hit = ids == m, near == m
                hits = (hit, hit, near_hit, near_hit)
                values = [jnp.where(hits[q], traits[q, m], values[q]) for q in range(4)]
            inside = ids >= 0
            cond[z, :, part] = values[0]
            rate_s[z, :, part] = jnp.where(inside, TIME_STEP / jnp.where(inside, values[1], 1.0), 0.0)
            mod[z + 1, :, part] = values[2] * inverse_shift[:, 0:cols]
            strain[z + 1, :, part] = values[3]
            mask[z + 1, :, part] = jnp.where(near >= 0, 1.0, 0.0)
            power = jnp.zeros(ids.shape, jnp.float32)
            for t in range(tiles):
                power = jnp.where(patches == t, power_table[t], power)
            pow_s[z, :, part] = power
        return 0

    lax.fori_loop(0, layers, prepare, 0, unroll=2)

    def conduct(a, b):
        return 2.0 * a * b / jnp.maximum(a + b, 0.25)

    def heat(z, flow_below, source, first):
        centre = source[z]
        if first:
            own_cond = cond[z]
            along_x = conduct(own_cond, shift(own_cond, 0, 1))
            along_y = conduct(own_cond, shift(own_cond, 1, 1))
            along_z = conduct(own_cond, cond[z + 1])
            gx_s[z], gy_s[z], gz_s[z] = along_x, along_y, along_z
        else:
            along_x, along_y, along_z = gx_s[z], gy_s[z], gz_s[z]
        flow_x = along_x * (shift(centre, 0, 1) - centre)
        flow_y = along_y * (shift(centre, 1, 1) - centre)
        flow_z = along_z * (source[jnp.minimum(z + 1, layers - 1)] - centre)
        flux = flow_x - shift(flow_x, 0, -1) + flow_y - shift(flow_y, 1, -1) + flow_z - flow_below
        return centre + rate_s[z] * (flux + pow_s[z]), flow_z

    def first_step(z, flow_below):
        temp2[z], flow_z = heat(z, flow_below, temp, True)
        return flow_z

    blank = mod[0]
    lax.fori_loop(0, layers, first_step, cond[layers], unroll=4)

    def second_step(z, flow_below):
        value, flow_z = heat(z, flow_below, temp2, False)
        warmed[z] = value[HALO : HALO + rows, 0:cols]
        strain[z + 1] = strain[z + 1] * value[kept]
        return flow_z

    lax.fori_loop(0, layers, second_step, cond[layers], unroll=4)
    results = [pltpu.make_async_copy(warmed, warmed_out, out_sem.at[0])]
    results[0].start()


    def matrix_planes(p):
        f = mod[p]
        sx, sy, sxsy, ex, ey, cross = matrix_parts(f)
        z0, z1 = diag_z(f, sx, sy, sxsy)
        x0, x1 = diag_x(f, sx, sy, sxsy)
        y0, y1 = diag_y(f, sx, sy, sxsy)
        zero = jnp.zeros_like(f)
        return (
            (z0, x0, y0, zero, zero, 0.125 * cross),
            (z1, x1, y1, zero, zero, (1.0 / 18.0) * cross),
            (zero, zero, zero, ex, ey, zero),
        )

    def matrix_emit(p, out, extra):
        diagonal = (ANCHOR + K_TOTAL) * mod[p] - 1.0
        for c in range(6):
            mats[c, p] = out[c] + diagonal if c < 3 else out[c]
        return extra

    stream(layers, 6, blank, matrix_planes, matrix_emit, 0)

    def fold(inner):
        result = inner[0:8]
        for r in range(8, rows, 8):
            result = result + inner[r : r + 8]
        return result

    tile = mod[0, 0:8, 0:cols]

    def load_planes(p):
        m, s = mod[p], strain[p]
        parts = [gradient_stencil(f) for f in (s, m, m * s)]
        return tuple(tuple(a for part in parts for a in part[i]) for i in range(3))

    def load_emit(p, out, acc):
        m, s, inside = mod[p], strain[p], mask[p]
        for c in range(3):
            value = -inside * (m * out[c] + s * out[3 + c] + out[6 + c])
            v[0, c, p] = value
            inner = value[inner_rows, 0:cols]
            vown[0, c, p] = inner
            acc = acc + fold(inner * inner)
        return acc

    moment_s[0] = stream(layers, 9, blank, load_planes, load_emit, tile)

    def shares(k):
        found = []
        for step in range(1, nz):
            there = lax.rem(iz + step, nz)
            found.append(
                pltpu.make_async_remote_copy(
                    src_ref=vown.at[k, :, pl.ds(1 + there * share, share)],
                    dst_ref=vrecv.at[k, step - 1],
                    send_sem=vsend_sem.at[k, step - 1], recv_sem=vrecv_sem.at[k, step - 1],
                    device_id=(ix, iy, there), device_id_type=MESH,
                )
            )
        return found

    def share_basis(k):
        for copy in shares(k):
            copy.start()

    share_basis(0)

    def apply(k, width):
        def planes(p):
            m = mod[p]
            u = [v[k, c, p] for c in range(3)]
            first = vector_stencil(*u, width)
            second = vector_stencil(*[m * f for f in u], width)
            return tuple(a + b for a, b in zip(first, second))

        def emit(p, out, acc):
            m = mod[p, :, 0:width]
            u = [v[k, c, p, :, 0:width] for c in range(3)]
            zz, xx, yy, zx, zy, xy = [mats[c, p, :, 0:width] for c in range(6)]
            grown = (
                zz * u[0] + zx * u[1] + zy * u[2],
                zx * u[0] + xx * u[1] + xy * u[2],
                zy * u[0] + xy * u[1] + yy * u[2],
            )
            odd, even = acc
            for c in range(3):
                value = grown[c] - m * out[c] - out[3 + c]
                if width > cols:
                    value = mask[p] * value
                    v[k + 1, c, p] = value
                inner = value[inner_rows, 0:cols]
                vown[k + 1, c, p] = inner
                odd = odd + fold(inner * vown[k, c, p])
                even = even + fold(inner * inner)
            return odd, even

        odd, even = stream(layers, 6, mod[0, :, 0:width], planes, emit, (tile, tile))
        moment_s[2 * k + 1] = odd
        moment_s[2 * k + 2] = even

    def grow(k, _):
        apply(k, 2 * cols)
        share_basis(k + 1)
        return 0

    lax.fori_loop(0, ITERS - 1, grow, 0)
    apply(ITERS - 1, cols)

    lane8 = lax.broadcasted_iota(jnp.int32, (1, cols), 1)
    row = jnp.zeros((1, cols), jnp.float32)
    for k in range(2 * ITERS):
        line = jnp.sum(moment_s[k], axis=0, keepdims=True)
        row = jnp.where(lane8 == k, jnp.sum(line, axis=1, keepdims=True), row)
    red_src[...] = row
    red_buf[me] = row

    def spread(k):
        there = lax.rem(me + k, total)
        return pltpu.make_async_remote_copy(
            src_ref=red_src, dst_ref=red_buf.at[me], send_sem=rsend_sem.at[k],
            recv_sem=rrecv_sem.at[k], device_id=coords(there), device_id_type=MESH,
        )

    def collect(k):
        there = lax.rem(me + total - k, total)
        return pltpu.make_async_remote_copy(
            src_ref=red_src, dst_ref=red_buf.at[there], send_sem=rsend_sem.at[k],
            recv_sem=rrecv_sem.at[k], device_id=coords(there), device_id_type=MESH,
        )

    def start(k, _):
        spread(k).start()
        return 0

    def finish(k, _):
        collect(k).wait_recv()
        return 0

    def sent(k, _):
        spread(k).wait_send()
        return 0

    lax.fori_loop(1, total, start, 0)
    share_basis(ITERS)
    lax.fori_loop(1, total, finish, 0)

    def add(k, acc):
        return acc + red_buf[k]

    summed = lax.fori_loop(0, total, add, jnp.zeros((1, cols), jnp.float32))
    m = [
        jnp.sum(jnp.where(lane8 == k, summed, 0.0), axis=1, keepdims=True) for k in range(2 * ITERS)
    ]

    def inner(a, b):
        value = None
        for i, x in enumerate(a):
            for j, y in enumerate(b):
                if x is not None and y is not None:
                    term = x * y * m[i + j]
                    value = term if value is None else value + term
        return value

    def plus(a, factor, b):
        out = []
        for x, y in zip(a, b):
            if y is None:
                out.append(x)
            else:
                out.append(factor * y if x is None else x + factor * y)
        return out

    one = jnp.ones((1, 1), jnp.float32)
    size = ITERS + 1
    res = [one] + [None] * ITERS
    dire = list(res)
    sol = [None] * size
    rr = m[0]
    for number in range(ITERS):
        image = plus(list(dire), 1.0, [None] + dire[:-1])
        alpha = rr / inner(dire, image)
        sol = plus(sol, alpha, dire)
        res = plus(res, -alpha, image)
        if number + 1 < ITERS:
            new = inner(res, res)
            dire = plus(res, new / rr, dire)
            rr = new
    res = [shift_scalar * x for x in res]

    for step in range(nz):
        where = pl.ds(pl.multiple_of(lax.rem(iz + nz - step, nz) * cols, cols), cols)
        if step:
            for k in range(size):
                shares(k)[step - 1].wait_recv()

        def combine(z, _, step=step, where=where):
            for c in range(3):
                if step == 0:
                    parts = [vown[k, c, 1 + iz * share + z] for k in range(size)]
                else:
                    parts = [vrecv[k, step - 1, c, z] for k in range(size)]
                total_s = sol[0] * parts[0]
                total_r = res[0] * parts[0]
                for k in range(1, size):
                    if sol[k] is not None:
                        total_s = total_s + sol[k] * parts[k]
                    total_r = total_r + res[k] * parts[k]
                solution[step, c, z] = total_s
                residual[step, c, z] = total_r
            return 0

        lax.fori_loop(0, share, combine, 0, unroll=2)
        for index, (a, b) in enumerate(((solution, solution_out), (residual, residual_out))):
            results.append(
                pltpu.make_async_copy(
                    a.at[step], b.at[:, :, :, where], out_sem.at[1 + 2 * step + index]
                )
            )
            results[-1].start()

    for target, _, copies, _, _ in moves:
        @pl.when(target)
        def _(copies=copies):
            for copy in copies:
                copy.wait_send()
    for k in range(ITERS + 1):
        for copy in shares(k):
            copy.wait_send()
    lax.fori_loop(1, total, sent, 0)
    for copy in results:
        copy.wait()


def per_device(sizes, *arrays):
    nx, ny, nz = sizes
    layers, rows, cols = arrays[0].shape
    total = nx * ny * nz
    share = layers // nz
    ext = (rows + 2 * HALO, 2 * cols)
    f32, i32 = jnp.float32, jnp.int32
    vmem = pltpu.VMEM
    dma = pltpu.SemaphoreType.DMA
    out = jax.ShapeDtypeStruct((3, share, rows, cols * nz), f32)
    plane = vmem((layers, *ext), f32)
    kept = (rows + 2 * EDGE, 2 * cols)
    padded = vmem((layers + 2, *kept), f32)
    half = vmem((nz, 3, share, rows, cols), f32)
    return pl.pallas_call(
        functools.partial(kernel, sizes),
        out_shape=(jax.ShapeDtypeStruct((layers, rows, cols), f32), out, out),
        in_specs=[pl.BlockSpec(memory_space=pltpu.HBM)] * 5,
        out_specs=[pl.BlockSpec(memory_space=pl.ANY)] * 3,
        scratch_shapes=[
            pltpu.SMEM(arrays[3].shape, f32), pltpu.SMEM(arrays[4].shape, f32), dma((2,)),
            vmem((layers, rows, cols), f32), half, half,
            vmem((ITERS + 1, 3, layers + 1, rows, cols), f32),
            vmem((2 * ITERS + 1, 8, cols), f32), dma((1 + 2 * nz,)),
            plane, plane, vmem((layers, *ext), i32), vmem((layers, *ext), i32),
            vmem((layers + 1, *ext), f32), padded, padded, padded,
            plane, plane, plane, plane, plane,
            vmem((6, layers + 1, *kept), f32),
            vmem((ITERS, 3, layers + 2, *kept), f32),
            vmem((ITERS + 1, nz - 1, 3, share, rows, cols), f32),
            vmem((2, rows, cols), f32), vmem((2, 2, rows, cols), i32),
            vmem((2, ext[0], cols), f32), vmem((2, 2, ext[0], cols), i32),
            vmem((1, cols), f32), vmem((total, 1, cols), f32),
            dma((3,)), dma((8, 3)), dma((8, 3)),
            dma((ITERS + 1, nz - 1)), dma((ITERS + 1, nz - 1)), dma((total,)), dma((total,)),
        ],
        compiler_params=pltpu.CompilerParams(
            collective_id=0, has_side_effects=True, vmem_limit_bytes=40 * 1024 * 1024
        ),
    )(*[pltpu.with_memory_space_constraint(a, pltpu.HBM) for a in arrays])


def solution(mesh):
    sizes = tuple(mesh.shape[axis] for axis in ("gx", "gy", "gz"))
    split = P(None, "gx", ("gy", "gz"))
    out = P(None, "gz", "gx", "gy")
    return jax.shard_map(
        functools.partial(per_device, sizes),
        mesh=mesh,
        in_specs=(split, split, split, P(), P()),
        out_specs=(split, out, out),
        check_vma=False,
    )
```

```python
import functools

import jax
import jax.numpy as jnp
from jax import lax
from jax.experimental import pallas as pl
from jax.experimental.pallas import tpu as pltpu
from jax.sharding import PartitionSpec as P

ITERS = 3
HALO = 8
REACH = 6
EDGE = 4
TIME_STEP = 0.03
ANCHOR = 0.5
K_TOTAL = 4 * 0.25 + 4 * 0.125 + 2 * (0.75 + 4 * 0.25 + 4 * 5.0 / 36.0)
MESH = pl.DeviceIdType.MESH
DIRECTIONS = [(dx, dc) for dx in (-1, 0, 1) for dc in (-1, 0, 1) if (dx, dc) != (0, 0)]


def shift(f, axis, step):
    return pltpu.roll(f, (-step) % f.shape[axis], axis)


def sums(f, axis):
    after, before = shift(f, axis, 1), shift(f, axis, -1)
    return after + before, after - before


def matrix_parts(f, width=None):
    sy, dy = sums(f, 1)
    if width is not None:
        f, sy, dy = f[:, :width], sy[:, :width], dy[:, :width]
    sx, dx = sums(f, 0)
    sxsy, dxsy = sums(sy, 0)
    sxdy, dxdy = sums(dy, 0)
    return sx, sy, sxsy, dx * 0.125 + dxsy * (1.0 / 18.0), dy * 0.125 + sxdy * (1.0 / 18.0), dxdy


def diag_z(f, sx, sy, sxsy):
    near = 0.25 * (sx + sy)
    return near + 0.125 * sxsy, 0.75 * f + near + (5.0 / 36.0) * sxsy


def diag_x(f, sx, sy, sxsy):
    near = 0.25 * sy
    return 0.75 * sx + near + 0.25 * sxsy, 0.25 * (f + sx) + 0.125 * sy + (5.0 / 36.0) * sxsy


def diag_y(f, sx, sy, sxsy):
    near = 0.25 * sx
    return 0.75 * sy + near + 0.25 * sxsy, 0.25 * (f + sy) + 0.125 * sx + (5.0 / 36.0) * sxsy


def vector_stencil(uz, ux, uy, width):
    sx, sy, sxsy, ex, ey, _ = matrix_parts(uz, width)
    uz, ux_in, uy_in = uz[:, :width], ux[:, :width], uy[:, :width]
    z0, z1 = diag_z(uz, sx, sy, sxsy)
    dif_x, dif_y = ex, ey
    sx, sy, sxsy, ex, _, cross_x = matrix_parts(ux, width)
    x0, x1 = diag_x(ux_in, sx, sy, sxsy)
    dif_z = ex
    sx, sy, sxsy, _, ey, cross_y = matrix_parts(uy, width)
    y0, y1 = diag_y(uy_in, sx, sy, sxsy)
    dif_z = dif_z + ey
    x0, x1 = x0 + 0.125 * cross_y, x1 + (1.0 / 18.0) * cross_y
    y0, y1 = y0 + 0.125 * cross_x, y1 + (1.0 / 18.0) * cross_x
    return (z0, x0, y0), (z1, x1, y1), (dif_z, dif_x, dif_y)


def gradient_stencil(f):
    sy, dy = sums(f, 1)
    sx, dx = sums(f, 0)
    sxsy, dxsy = sums(sy, 0)
    sxdy, _ = sums(dy, 0)
    zero = jnp.zeros_like(f)
    return (
        (zero, 0.5 * dx + 0.25 * dxsy, 0.5 * dy + 0.25 * sxdy),
        (zero, 0.25 * dx + (1.0 / 6.0) * dxsy, 0.25 * dy + (1.0 / 6.0) * sxdy),
        (0.5 * f + 0.25 * (sx + sy) + (1.0 / 6.0) * sxsy, zero, zero),
    )


def stream(layers, count, zero, planes, emit, extra):
    def body(p, carry):
        held, below, extra = carry
        same, both, diff = planes(p)
        out = [h + b + d for h, b, d in zip(held, both, diff)]
        extra = emit(p - 1, out, extra)
        held = [w + s for w, s in zip(below, same)]
        below = [b - d for b, d in zip(both, diff)]
        return held, below, extra

    zeros = [zero] * count
    return lax.fori_loop(1, layers + 2, body, (zeros, list(zeros), extra), unroll=4)[2]


def kernel(
    sizes,
    kelvin, label, patch, traits_in, power_in,
    warmed_out, solution_out, residual_out,
    traits, power_table, table_sem, warmed, solution, residual, vown, moment_s, out_sem,
    temp, temp2, lab, pat, cond, mod, strain, mask, gx_s, gy_s, gz_s, rate_s, pow_s, mats,
    v, vrecv, pack_f, pack_i, got_f, got_i, red_src, red_buf,
    local_sem, send_sem, recv_sem, vsend_sem, vrecv_sem, rsend_sem, rrecv_sem,
):
    nx, ny, nz = sizes
    nc, total = ny * nz, nx * ny * nz
    layers, rows, cols = kelvin.shape
    share = layers // nz
    full_rows = rows + 2 * HALO
    shape = (full_rows, 2 * cols)
    kept = slice(HALO - EDGE, HALO + rows + EDGE)
    inner_rows = slice(EDGE, EDGE + rows)
    ix, iy, iz = lax.axis_index("gx"), lax.axis_index("gy"), lax.axis_index("gz")
    ic = iy * nz + iz
    me = ix * nc + ic

    def coords(flat):
        return (flat // nc, (flat % nc) // nz, flat % nz)

    barrier = pltpu.get_barrier_semaphore()

    def greet(k, _):
        pl.semaphore_signal(
            barrier, inc=1, device_id=coords(lax.rem(me + k, total)), device_id_type=MESH
        )
        return 0

    lax.fori_loop(1, total, greet, 0)

    own = (slice(None), pl.ds(HALO, rows), pl.ds(0, cols))
    local = [
        pltpu.make_async_copy(a, b.at[own], local_sem.at[i])
        for i, (a, b) in enumerate(((kelvin, temp), (label, lab), (patch, pat)))
    ]
    tables = [
        pltpu.make_async_copy(traits_in, traits, table_sem.at[0]),
        pltpu.make_async_copy(power_in, power_table, table_sem.at[1]),
    ]
    for copy in local + tables:
        copy.start()

    sources = (kelvin, label, patch)
    pl.semaphore_wait(barrier, total - 1)

    def transfers(number):
        dx, dc = DIRECTIONS[number]
        there = (lax.rem(ix + dx + nx, nx) * nc) + lax.rem(ic + dc + nc, nc)
        target = jnp.logical_and(
            jnp.logical_and(ix + dx >= 0, ix + dx < nx), jnp.logical_and(ic + dc >= 0, ic + dc < nc)
        )
        origin = jnp.logical_and(
            jnp.logical_and(ix - dx >= 0, ix - dx < nx), jnp.logical_and(ic - dc >= 0, ic - dc < nc)
        )
        if dx == 0:
            from_rows, to_rows = pl.ds(0, rows), pl.ds(HALO, rows)
        elif dx == 1:
            from_rows, to_rows = pl.ds(rows - REACH, REACH), pl.ds(HALO - REACH, REACH)
        else:
            from_rows, to_rows = pl.ds(0, REACH), pl.ds(HALO + rows, REACH)
        if dc == 0:
            pairs = [
                (ref.at[:, from_rows, :], ext.at[:, to_rows, pl.ds(0, cols)])
                for ref, ext in zip(sources, (temp, lab, pat))
            ]
        else:
            side = (dc + 1) // 2
            pairs = [(pack_f.at[side, from_rows, :], got_f.at[side, to_rows, :])]
            pairs += [
                (pack_i.at[side, i, from_rows, :], got_i.at[side, i, to_rows, :]) for i in (0, 1)
            ]
        copies = [
            pltpu.make_async_remote_copy(
                src_ref=a, dst_ref=b, send_sem=send_sem.at[number, i],
                recv_sem=recv_sem.at[number, i], device_id=coords(there), device_id_type=MESH,
            )
            for i, (a, b) in enumerate(pairs)
        ]
        return target, origin, copies, to_rows, dc

    moves = [transfers(i) for i in range(len(DIRECTIONS))]
    for target, _, copies, _, dc in moves:
        if dc != 0:
            continue

        @pl.when(target)
        def _(copies=copies):
            for copy in copies:
                copy.start()

    lane = lax.broadcasted_iota(jnp.int32, (rows, cols), 1)
    for copy in local:
        copy.wait()
    for side in (0, 1):
        for index, ref in enumerate((temp, lab, pat)):
            packed = jnp.zeros((rows, cols), ref.dtype)
            for z in range(layers):
                amount = (HALO * z + (HALO if side else 0)) % cols
                piece = ref[(z, *own[1:])]
                piece = pltpu.roll(piece, amount, 1) if amount else piece
                packed = jnp.where(lane // HALO == z, piece, packed)
            if index == 0:
                pack_f[side] = packed
            else:
                pack_i[side, index - 1] = packed

    for target, _, copies, _, dc in moves:
        if dc == 0:
            continue

        @pl.when(target)
        def _(copies=copies):
            for copy in copies:
                copy.start()

    for _, origin, _, to_rows, dc in moves:
        @pl.when(jnp.logical_not(origin))
        def _(to_rows=to_rows, dc=dc):
            if dc == 0:
                block = (layers, to_rows.size, cols)
                temp[:, to_rows, 0:cols] = jnp.zeros(block, jnp.float32)
                lab[:, to_rows, 0:cols] = jnp.full(block, -1, jnp.int32)
                pat[:, to_rows, 0:cols] = jnp.zeros(block, jnp.int32)
            else:
                side = (dc + 1) // 2
                block = (to_rows.size, cols)
                got_f[side, to_rows, :] = jnp.zeros(block, jnp.float32)
                got_i[side, 0, to_rows, :] = jnp.full(block, -1, jnp.int32)
                got_i[side, 1, to_rows, :] = jnp.zeros(block, jnp.int32)

    empty = jnp.zeros(shape, jnp.float32)
    blank_kept = jnp.zeros((rows + 2 * EDGE, 2 * cols), jnp.float32)
    for end in (0, layers + 1):
        for ref in (mod, strain, mask):
            ref[end] = blank_kept
        for k in range(ITERS):
            for c in range(3):
                v[k, c, end] = blank_kept
    for c in range(6):
        mats[c, 0] = blank_kept
    cond[layers] = empty

    for copy in tables:
        copy.wait()
    shift_scalar = 3.0 * (traits[2, 0] + traits[2, 1] + traits[2, 2] + traits[2, 3])
    inverse_shift = 1.0 / jnp.full((1, 2 * cols), shift_scalar, jnp.float32)

    for _, origin, copies, _, _ in moves:
        @pl.when(origin)
        def _(copies=copies):
            for copy in copies:
                copy.wait_recv()

    halo_lane = lax.broadcasted_iota(jnp.int32, (full_rows, cols), 1)
    materials = traits.shape[1]
    tiles = power_table.shape[0]

    def prepare(z, _):
        def unpack(left, right, outside):
            left = pltpu.roll(left, lax.rem(2 * cols - HALO - HALO * z, cols), 1)
            right = pltpu.roll(right, lax.rem(cols - HALO * z, cols), 1)
            rest = jnp.where(halo_lane >= cols - HALO, left, outside)
            return jnp.where(halo_lane < HALO, right, rest)

        temp[z, :, cols:] = unpack(got_f[1], got_f[0], jnp.float32(0.0))
        label_halo = unpack(got_i[1, 0], got_i[0, 0], jnp.int32(-1))
        patch_halo = unpack(got_i[1, 1], got_i[0, 1], jnp.int32(0))
        for part, ids, patches in (
            (pl.ds(0, cols), lab[z, :, 0:cols], pat[z, :, 0:cols]),
            (pl.ds(cols, cols), label_halo, patch_halo),
        ):
            near = ids[kept]
            values = [jnp.zeros(a.shape, jnp.float32) for a in (ids, ids, near, near)]
            for m in range(materials):
                hit, near_hit = ids == m, near == m
                hits = (hit, hit, near_hit, near_hit)
                values = [jnp.where(hits[q], traits[q, m], values[q]) for q in range(4)]
            inside = ids >= 0
            cond[z, :, part] = values[0]
            rate_s[z, :, part] = jnp.where(inside, TIME_STEP / jnp.where(inside, values[1], 1.0), 0.0)
            mod[z + 1, :, part] = values[2] * inverse_shift[:, 0:cols]
            strain[z + 1, :, part] = values[3]
            mask[z + 1, :, part] = jnp.where(near >= 0, 1.0, 0.0)
            power = jnp.zeros(ids.shape, jnp.float32)
            for t in range(tiles):
                power = jnp.where(patches == t, power_table[t], power)
            pow_s[z, :, part] = power
        return 0

    lax.fori_loop(0, layers, prepare, 0, unroll=2)

    def conduct(a, b):
        return 2.0 * a * b / jnp.maximum(a + b, 0.25)

    def heat(z, flow_below, source, first):
        centre = source[z]
        if first:
            own_cond = cond[z]
            along_x = conduct(own_cond, shift(own_cond, 0, 1))
            along_y = conduct(own_cond, shift(own_cond, 1, 1))
            along_z = conduct(own_cond, cond[z + 1])
            gx_s[z], gy_s[z], gz_s[z] = along_x, along_y, along_z
        else:
            along_x, along_y, along_z = gx_s[z], gy_s[z], gz_s[z]
        flow_x = along_x * (shift(centre, 0, 1) - centre)
        flow_y = along_y * (shift(centre, 1, 1) - centre)
        flow_z = along_z * (source[jnp.minimum(z + 1, layers - 1)] - centre)
        flux = flow_x - shift(flow_x, 0, -1) + flow_y - shift(flow_y, 1, -1) + flow_z - flow_below
        return centre + rate_s[z] * (flux + pow_s[z]), flow_z

    def first_step(z, flow_below):
        temp2[z], flow_z = heat(z, flow_below, temp, True)
        return flow_z

    blank = mod[0]
    lax.fori_loop(0, layers, first_step, cond[layers], unroll=4)

    def second_step(z, flow_below):
        value, flow_z = heat(z, flow_below, temp2, False)
        warmed[z] = value[HALO : HALO + rows, 0:cols]
        strain[z + 1] = strain[z + 1] * value[kept]
        return flow_z

    lax.fori_loop(0, layers, second_step, cond[layers], unroll=4)
    results = [pltpu.make_async_copy(warmed, warmed_out, out_sem.at[0])]
    results[0].start()


    def matrix_planes(p):
        f = mod[p]
        sx, sy, sxsy, ex, ey, cross = matrix_parts(f)
        z0, z1 = diag_z(f, sx, sy, sxsy)
        x0, x1 = diag_x(f, sx, sy, sxsy)
        y0, y1 = diag_y(f, sx, sy, sxsy)
        zero = jnp.zeros_like(f)
        return (
            (z0, x0, y0, zero, zero, 0.125 * cross),
            (z1, x1, y1, zero, zero, (1.0 / 18.0) * cross),
            (zero, zero, zero, ex, ey, zero),
        )

    def matrix_emit(p, out, extra):
        diagonal = (ANCHOR + K_TOTAL) * mod[p] - 1.0
        for c in range(6):
            mats[c, p] = out[c] + diagonal if c < 3 else out[c]
        return extra

    stream(layers, 6, blank, matrix_planes, matrix_emit, 0)

    def fold(inner):
        result = inner[0:8]
        for r in range(8, rows, 8):
            result = result + inner[r : r + 8]
        return result

    tile = mod[0, 0:8, 0:cols]

    def load_planes(p):
        m, s = mod[p], strain[p]
        parts = [gradient_stencil(f) for f in (s, m, m * s)]
        return tuple(tuple(a for part in parts for a in part[i]) for i in range(3))

    def load_emit(p, out, acc):
        m, s, inside = mod[p], strain[p], mask[p]
        for c in range(3):
            value = -inside * (m * out[c] + s * out[3 + c] + out[6 + c])
            v[0, c, p] = value
            inner = value[inner_rows, 0:cols]
            vown[0, c, p] = inner
            acc = acc + fold(inner * inner)
        return acc

    moment_s[0] = stream(layers, 9, blank, load_planes, load_emit, tile)

    def shares(k):
        found = []
        for step in range(1, nz):
            there = lax.rem(iz + step, nz)
            found.append(
                pltpu.make_async_remote_copy(
                    src_ref=vown.at[k, :, pl.ds(1 + there * share, share)],
                    dst_ref=vrecv.at[k, step - 1],
                    send_sem=vsend_sem.at[k, step - 1], recv_sem=vrecv_sem.at[k, step - 1],
                    device_id=(ix, iy, there), device_id_type=MESH,
                )
            )
        return found

    def share_basis(k):
        for copy in shares(k):
            copy.start()

    share_basis(0)

    def apply(k, width):
        def planes(p):
            m = mod[p]
            u = [v[k, c, p] for c in range(3)]
            first = vector_stencil(*u, width)
            second = vector_stencil(*[m * f for f in u], width)
            return tuple(a + b for a, b in zip(first, second))

        def emit(p, out, acc):
            m = mod[p, :, 0:width]
            u = [v[k, c, p, :, 0:width] for c in range(3)]
            zz, xx, yy, zx, zy, xy = [mats[c, p, :, 0:width] for c in range(6)]
            grown = (
                zz * u[0] + zx * u[1] + zy * u[2],
                zx * u[0] + xx * u[1] + xy * u[2],
                zy * u[0] + xy * u[1] + yy * u[2],
            )
            odd, even = acc
            for c in range(3):
                value = grown[c] - m * out[c] - out[3 + c]
                if width > cols:
                    value = mask[p] * value
                    v[k + 1, c, p] = value
                inner = value[inner_rows, 0:cols]
                vown[k + 1, c, p] = inner
                odd = odd + fold(inner * vown[k, c, p])
                even = even + fold(inner * inner)
            return odd, even

        odd, even = stream(layers, 6, mod[0, :, 0:width], planes, emit, (tile, tile))
        moment_s[2 * k + 1] = odd
        moment_s[2 * k + 2] = even

    def grow(k, _):
        apply(k, 2 * cols)
        share_basis(k + 1)
        return 0

    lax.fori_loop(0, ITERS - 1, grow, 0)
    apply(ITERS - 1, cols)

    lane8 = lax.broadcasted_iota(jnp.int32, (1, cols), 1)
    row = jnp.zeros((1, cols), jnp.float32)
    for k in range(2 * ITERS):
        line = jnp.sum(moment_s[k], axis=0, keepdims=True)
        row = jnp.where(lane8 == k, jnp.sum(line, axis=1, keepdims=True), row)
    red_src[...] = row
    red_buf[me] = row

    def spread(k):
        there = lax.rem(me + k, total)
        return pltpu.make_async_remote_copy(
            src_ref=red_src, dst_ref=red_buf.at[me], send_sem=rsend_sem.at[k],
            recv_sem=rrecv_sem.at[k], device_id=coords(there), device_id_type=MESH,
        )

    def collect(k):
        there = lax.rem(me + total - k, total)
        return pltpu.make_async_remote_copy(
            src_ref=red_src, dst_ref=red_buf.at[there], send_sem=rsend_sem.at[k],
            recv_sem=rrecv_sem.at[k], device_id=coords(there), device_id_type=MESH,
        )

    def start(k, _):
        spread(k).start()
        return 0

    def finish(k, _):
        collect(k).wait_recv()
        return 0

    def sent(k, _):
        spread(k).wait_send()
        return 0

    lax.fori_loop(1, total, start, 0)
    share_basis(ITERS)
    lax.fori_loop(1, total, finish, 0)

    def add(k, acc):
        return acc + red_buf[k]

    summed = lax.fori_loop(0, total, add, jnp.zeros((1, cols), jnp.float32))
    m = [
        jnp.sum(jnp.where(lane8 == k, summed, 0.0), axis=1, keepdims=True) for k in range(2 * ITERS)
    ]

    def inner(a, b):
        value = None
        for i, x in enumerate(a):
            for j, y in enumerate(b):
                if x is not None and y is not None:
                    term = x * y * m[i + j]
                    value = term if value is None else value + term
        return value

    def plus(a, factor, b):
        out = []
        for x, y in zip(a, b):
            if y is None:
                out.append(x)
            else:
                out.append(factor * y if x is None else x + factor * y)
        return out

    one = jnp.ones((1, 1), jnp.float32)
    size = ITERS + 1
    res = [one] + [None] * ITERS
    dire = list(res)
    sol = [None] * size
    rr = m[0]
    for number in range(ITERS):
        image = plus(list(dire), 1.0, [None] + dire[:-1])
        alpha = rr / inner(dire, image)
        sol = plus(sol, alpha, dire)
        res = plus(res, -alpha, image)
        if number + 1 < ITERS:
            new = inner(res, res)
            dire = plus(res, new / rr, dire)
            rr = new
    res = [shift_scalar * x for x in res]

    for step in range(nz):
        where = pl.ds(pl.multiple_of(lax.rem(iz + nz - step, nz) * cols, cols), cols)
        if step:
            for k in range(size):
                shares(k)[step - 1].wait_recv()

        def combine(z, _, step=step, where=where):
            for c in range(3):
                if step == 0:
                    parts = [vown[k, c, 1 + iz * share + z] for k in range(size)]
                else:
                    parts = [vrecv[k, step - 1, c, z] for k in range(size)]
                total_s = sol[0] * parts[0]
                total_r = res[0] * parts[0]
                for k in range(1, size):
                    if sol[k] is not None:
                        total_s = total_s + sol[k] * parts[k]
                    total_r = total_r + res[k] * parts[k]
                solution[step, c, z] = total_s
                residual[step, c, z] = total_r
            return 0

        lax.fori_loop(0, share, combine, 0, unroll=2)
        for index, (a, b) in enumerate(((solution, solution_out), (residual, residual_out))):
            results.append(
                pltpu.make_async_copy(
                    a.at[step], b.at[:, :, :, where], out_sem.at[1 + 2 * step + index]
                )
            )
            results[-1].start()

    for target, _, copies, _, _ in moves:
        @pl.when(target)
        def _(copies=copies):
            for copy in copies:
                copy.wait_send()
    for k in range(ITERS + 1):
        for copy in shares(k):
            copy.wait_send()
    lax.fori_loop(1, total, sent, 0)
    for copy in results:
        copy.wait()


def per_device(sizes, *arrays):
    nx, ny, nz = sizes
    layers, rows, cols = arrays[0].shape
    total = nx * ny * nz
    share = layers // nz
    ext = (rows + 2 * HALO, 2 * cols)
    f32, i32 = jnp.float32, jnp.int32
    vmem = pltpu.VMEM
    dma = pltpu.SemaphoreType.DMA
    out = jax.ShapeDtypeStruct((3, share, rows, cols * nz), f32)
    plane = vmem((layers, *ext), f32)
    kept = (rows + 2 * EDGE, 2 * cols)
    padded = vmem((layers + 2, *kept), f32)
    half = vmem((nz, 3, share, rows, cols), f32)
    return pl.pallas_call(
        functools.partial(kernel, sizes),
        out_shape=(jax.ShapeDtypeStruct((layers, rows, cols), f32), out, out),
        in_specs=[pl.BlockSpec(memory_space=pltpu.HBM)] * 5,
        out_specs=[pl.BlockSpec(memory_space=pl.ANY)] * 3,
        scratch_shapes=[
            pltpu.SMEM(arrays[3].shape, f32), pltpu.SMEM(arrays[4].shape, f32), dma((2,)),
            vmem((layers, rows, cols), f32), half, half,
            vmem((ITERS + 1, 3, layers + 1, rows, cols), f32),
            vmem((2 * ITERS + 1, 8, cols), f32), dma((1 + 2 * nz,)),
            plane, plane, vmem((layers, *ext), i32), vmem((layers, *ext), i32),
            vmem((layers + 1, *ext), f32), padded, padded, padded,
            plane, plane, plane, plane, plane,
            vmem((6, layers + 1, *kept), f32),
            vmem((ITERS, 3, layers + 2, *kept), f32),
            vmem((ITERS + 1, nz - 1, 3, share, rows, cols), f32),
            vmem((2, rows, cols), f32), vmem((2, 2, rows, cols), i32),
            vmem((2, ext[0], cols), f32), vmem((2, 2, ext[0], cols), i32),
            vmem((1, cols), f32), vmem((total, 1, cols), f32),
            dma((3,)), dma((8, 3)), dma((8, 3)),
            dma((ITERS + 1, nz - 1)), dma((ITERS + 1, nz - 1)), dma((total,)), dma((total,)),
        ],
        compiler_params=pltpu.CompilerParams(
            collective_id=0, has_side_effects=True, vmem_limit_bytes=40 * 1024 * 1024
        ),
    )(*[pltpu.with_memory_space_constraint(a, pltpu.HBM) for a in arrays])


def solution(mesh):
    sizes = tuple(mesh.shape[axis] for axis in ("gx", "gy", "gz"))
    split = P(None, "gx", ("gy", "gz"))
    out = P(None, "gz", "gx", "gy")
    return jax.shard_map(
        functools.partial(per_device, sizes),
        mesh=mesh,
        in_specs=(split, split, split, P(), P()),
        out_specs=(split, out, out),
        check_vma=False,
    )
```

```python
import functools

import jax
import jax.numpy as jnp
from jax import lax
from jax.experimental import pallas as pl
from jax.experimental.pallas import tpu as pltpu
from jax.sharding import PartitionSpec as P

ITERS = 3
HALO = 8
REACH = 6
EDGE = 4
TIME_STEP = 0.03
ANCHOR = 0.5
K_TOTAL = 4 * 0.25 + 4 * 0.125 + 2 * (0.75 + 4 * 0.25 + 4 * 5.0 / 36.0)
MESH = pl.DeviceIdType.MESH
DIRECTIONS = [(dx, dc) for dx in (-1, 0, 1) for dc in (-1, 0, 1) if (dx, dc) != (0, 0)]


def shift(f, axis, step):
    return pltpu.roll(f, (-step) % f.shape[axis], axis)


def sums(f, axis):
    after, before = shift(f, axis, 1), shift(f, axis, -1)
    return after + before, after - before


def matrix_parts(f, width=None):
    sy, dy = sums(f, 1)
    if width is not None:
        f, sy, dy = f[:, :width], sy[:, :width], dy[:, :width]
    sx, dx = sums(f, 0)
    sxsy, dxsy = sums(sy, 0)
    sxdy, dxdy = sums(dy, 0)
    return sx, sy, sxsy, dx * 0.125 + dxsy * (1.0 / 18.0), dy * 0.125 + sxdy * (1.0 / 18.0), dxdy


def diag_z(f, sx, sy, sxsy):
    near = 0.25 * (sx + sy)
    return near + 0.125 * sxsy, 0.75 * f + near + (5.0 / 36.0) * sxsy


def diag_x(f, sx, sy, sxsy):
    near = 0.25 * sy
    return 0.75 * sx + near + 0.25 * sxsy, 0.25 * (f + sx) + 0.125 * sy + (5.0 / 36.0) * sxsy


def diag_y(f, sx, sy, sxsy):
    near = 0.25 * sx
    return 0.75 * sy + near + 0.25 * sxsy, 0.25 * (f + sy) + 0.125 * sx + (5.0 / 36.0) * sxsy


def vector_stencil(uz, ux, uy, width):
    sx, sy, sxsy, ex, ey, _ = matrix_parts(uz, width)
    uz, ux_in, uy_in = uz[:, :width], ux[:, :width], uy[:, :width]
    z0, z1 = diag_z(uz, sx, sy, sxsy)
    dif_x, dif_y = ex, ey
    sx, sy, sxsy, ex, _, cross_x = matrix_parts(ux, width)
    x0, x1 = diag_x(ux_in, sx, sy, sxsy)
    dif_z = ex
    sx, sy, sxsy, _, ey, cross_y = matrix_parts(uy, width)
    y0, y1 = diag_y(uy_in, sx, sy, sxsy)
    dif_z = dif_z + ey
    x0, x1 = x0 + 0.125 * cross_y, x1 + (1.0 / 18.0) * cross_y
    y0, y1 = y0 + 0.125 * cross_x, y1 + (1.0 / 18.0) * cross_x
    return (z0, x0, y0), (z1, x1, y1), (dif_z, dif_x, dif_y)


def gradient_stencil(f):
    sy, dy = sums(f, 1)
    sx, dx = sums(f, 0)
    sxsy, dxsy = sums(sy, 0)
    sxdy, _ = sums(dy, 0)
    zero = jnp.zeros_like(f)
    return (
        (zero, 0.5 * dx + 0.25 * dxsy, 0.5 * dy + 0.25 * sxdy),
        (zero, 0.25 * dx + (1.0 / 6.0) * dxsy, 0.25 * dy + (1.0 / 6.0) * sxdy),
        (0.5 * f + 0.25 * (sx + sy) + (1.0 / 6.0) * sxsy, zero, zero),
    )


def stream(layers, count, zero, planes, emit, extra):
    def body(p, carry):
        held, below, extra = carry
        same, both, diff = planes(p)
        out = [h + b + d for h, b, d in zip(held, both, diff)]
        extra = emit(p - 1, out, extra)
        held = [w + s for w, s in zip(below, same)]
        below = [b - d for b, d in zip(both, diff)]
        return held, below, extra

    zeros = [zero] * count
    return lax.fori_loop(1, layers + 2, body, (zeros, list(zeros), extra), unroll=4)[2]


def kernel(
    sizes,
    kelvin, label, patch, traits_in, power_in,
    warmed_out, solution_out, residual_out,
    traits, power_table, table_sem, warmed, solution, residual, vown, moment_s, out_sem,
    temp, temp2, lab, pat, cond, mod, strain, mask, gx_s, gy_s, gz_s, rate_s, pow_s, mats,
    v, vrecv, pack_f, pack_i, got_f, got_i, red_src, red_buf,
    local_sem, send_sem, recv_sem, vsend_sem, vrecv_sem, rsend_sem, rrecv_sem,
):
    nx, ny, nz = sizes
    nc, total = ny * nz, nx * ny * nz
    layers, rows, cols = kelvin.shape
    share = layers // nz
    full_rows = rows + 2 * HALO
    shape = (full_rows, 2 * cols)
    kept = slice(HALO - EDGE, HALO + rows + EDGE)
    inner_rows = slice(EDGE, EDGE + rows)
    ix, iy, iz = lax.axis_index("gx"), lax.axis_index("gy"), lax.axis_index("gz")
    ic = iy * nz + iz
    me = ix * nc + ic

    def coords(flat):
        return (flat // nc, (flat % nc) // nz, flat % nz)

    barrier = pltpu.get_barrier_semaphore()

    def greet(k, _):
        pl.semaphore_signal(
            barrier, inc=1, device_id=coords(lax.rem(me + k, total)), device_id_type=MESH
        )
        return 0

    lax.fori_loop(1, total, greet, 0, unroll=4)

    own = (slice(None), pl.ds(HALO, rows), pl.ds(0, cols))
    local = [
        pltpu.make_async_copy(a, b.at[own], local_sem.at[i])
        for i, (a, b) in enumerate(((kelvin, temp), (label, lab), (patch, pat)))
    ]
    tables = [
        pltpu.make_async_copy(traits_in, traits, table_sem.at[0]),
        pltpu.make_async_copy(power_in, power_table, table_sem.at[1]),
    ]
    for copy in local + tables:
        copy.start()

    sources = (kelvin, label, patch)
    pl.semaphore_wait(barrier, total - 1)

    def transfers(number):
        dx, dc = DIRECTIONS[number]
        there = (lax.rem(ix + dx + nx, nx) * nc) + lax.rem(ic + dc + nc, nc)
        target = jnp.logical_and(
            jnp.logical_and(ix + dx >= 0, ix + dx < nx), jnp.logical_and(ic + dc >= 0, ic + dc < nc)
        )
        origin = jnp.logical_and(
            jnp.logical_and(ix - dx >= 0, ix - dx < nx), jnp.logical_and(ic - dc >= 0, ic - dc < nc)
        )
        if dx == 0:
            from_rows, to_rows = pl.ds(0, rows), pl.ds(HALO, rows)
        elif dx == 1:
            from_rows, to_rows = pl.ds(rows - REACH, REACH), pl.ds(HALO - REACH, REACH)
        else:
            from_rows, to_rows = pl.ds(0, REACH), pl.ds(HALO + rows, REACH)
        if dc == 0:
            pairs = [
                (ref.at[:, from_rows, :], ext.at[:, to_rows, pl.ds(0, cols)])
                for ref, ext in zip(sources, (temp, lab, pat))
            ]
        else:
            side = (dc + 1) // 2
            pairs = [(pack_f.at[side, from_rows, :], got_f.at[side, to_rows, :])]
            pairs += [
                (pack_i.at[side, i, from_rows, :], got_i.at[side, i, to_rows, :]) for i in (0, 1)
            ]
        copies = [
            pltpu.make_async_remote_copy(
                src_ref=a, dst_ref=b, send_sem=send_sem.at[number, i],
                recv_sem=recv_sem.at[number, i], device_id=coords(there), device_id_type=MESH,
            )
            for i, (a, b) in enumerate(pairs)
        ]
        return target, origin, copies, to_rows, dc

    moves = [transfers(i) for i in range(len(DIRECTIONS))]
    for target, _, copies, _, dc in moves:
        if dc != 0:
            continue

        @pl.when(target)
        def _(copies=copies):
            for copy in copies:
                copy.start()

    lane = lax.broadcasted_iota(jnp.int32, (rows, cols), 1)
    for copy in local:
        copy.wait()
    for side in (0, 1):
        for index, ref in enumerate((temp, lab, pat)):
            packed = jnp.zeros((rows, cols), ref.dtype)
            for z in range(layers):
                amount = (HALO * z + (HALO if side else 0)) % cols
                piece = ref[(z, *own[1:])]
                piece = pltpu.roll(piece, amount, 1) if amount else piece
                packed = jnp.where(lane // HALO == z, piece, packed)
            if index == 0:
                pack_f[side] = packed
            else:
                pack_i[side, index - 1] = packed

    for target, _, copies, _, dc in moves:
        if dc == 0:
            continue

        @pl.when(target)
        def _(copies=copies):
            for copy in copies:
                copy.start()

    for _, origin, _, to_rows, dc in moves:
        @pl.when(jnp.logical_not(origin))
        def _(to_rows=to_rows, dc=dc):
            if dc == 0:
                block = (layers, to_rows.size, cols)
                temp[:, to_rows, 0:cols] = jnp.zeros(block, jnp.float32)
                lab[:, to_rows, 0:cols] = jnp.full(block, -1, jnp.int32)
                pat[:, to_rows, 0:cols] = jnp.zeros(block, jnp.int32)
            else:
                side = (dc + 1) // 2
                block = (to_rows.size, cols)
                got_f[side, to_rows, :] = jnp.zeros(block, jnp.float32)
                got_i[side, 0, to_rows, :] = jnp.full(block, -1, jnp.int32)
                got_i[side, 1, to_rows, :] = jnp.zeros(block, jnp.int32)

    empty = jnp.zeros(shape, jnp.float32)
    blank_kept = jnp.zeros((rows + 2 * EDGE, 2 * cols), jnp.float32)
    for end in (0, layers + 1):
        for ref in (mod, strain, mask):
            ref[end] = blank_kept
        for k in range(ITERS):
            for c in range(3):
                v[k, c, end] = blank_kept
    for c in range(6):
        mats[c, 0] = blank_kept
    cond[layers] = empty

    for copy in tables:
        copy.wait()
    shift_scalar = 3.0 * (traits[2, 0] + traits[2, 1] + traits[2, 2] + traits[2, 3])
    inverse_shift = 1.0 / jnp.full((1, 2 * cols), shift_scalar, jnp.float32)

    for _, origin, copies, _, _ in moves:
        @pl.when(origin)
        def _(copies=copies):
            for copy in copies:
                copy.wait_recv()

    halo_lane = lax.broadcasted_iota(jnp.int32, (full_rows, cols), 1)
    materials = traits.shape[1]
    tiles = power_table.shape[0]

    def prepare(z, _):
        def unpack(left, right, outside):
            left = pltpu.roll(left, lax.rem(2 * cols - HALO - HALO * z, cols), 1)
            right = pltpu.roll(right, lax.rem(cols - HALO * z, cols), 1)
            rest = jnp.where(halo_lane >= cols - HALO, left, outside)
            return jnp.where(halo_lane < HALO, right, rest)

        temp[z, :, cols:] = unpack(got_f[1], got_f[0], jnp.float32(0.0))
        label_halo = unpack(got_i[1, 0], got_i[0, 0], jnp.int32(-1))
        patch_halo = unpack(got_i[1, 1], got_i[0, 1], jnp.int32(0))
        for part, ids, patches in (
            (pl.ds(0, cols), lab[z, :, 0:cols], pat[z, :, 0:cols]),
            (pl.ds(cols, cols), label_halo, patch_halo),
        ):
            near = ids[kept]
            values = [jnp.zeros(a.shape, jnp.float32) for a in (ids, ids, near, near)]
            for m in range(materials):
                hit, near_hit = ids == m, near == m
                hits = (hit, hit, near_hit, near_hit)
                values = [jnp.where(hits[q], traits[q, m], values[q]) for q in range(4)]
            inside = ids >= 0
            cond[z, :, part] = values[0]
            rate_s[z, :, part] = jnp.where(inside, TIME_STEP / jnp.where(inside, values[1], 1.0), 0.0)
            mod[z + 1, :, part] = values[2] * inverse_shift[:, 0:cols]
            strain[z + 1, :, part] = values[3]
            mask[z + 1, :, part] = jnp.where(near >= 0, 1.0, 0.0)
            power = jnp.zeros(ids.shape, jnp.float32)
            for t in range(tiles):
                power = jnp.where(patches == t, power_table[t], power)
            pow_s[z, :, part] = power
        return 0

    lax.fori_loop(0, layers, prepare, 0, unroll=4)

    def conduct(a, b):
        return 2.0 * a * b / jnp.maximum(a + b, 0.25)

    def heat(z, flow_below, source, first):
        centre = source[z]
        if first:
            own_cond = cond[z]
            along_x = conduct(own_cond, shift(own_cond, 0, 1))
            along_y = conduct(own_cond, shift(own_cond, 1, 1))
            along_z = conduct(own_cond, cond[z + 1])
            gx_s[z], gy_s[z], gz_s[z] = along_x, along_y, along_z
        else:
            along_x, along_y, along_z = gx_s[z], gy_s[z], gz_s[z]
        flow_x = along_x * (shift(centre, 0, 1) - centre)
        flow_y = along_y * (shift(centre, 1, 1) - centre)
        flow_z = along_z * (source[jnp.minimum(z + 1, layers - 1)] - centre)
        flux = flow_x - shift(flow_x, 0, -1) + flow_y - shift(flow_y, 1, -1) + flow_z - flow_below
        return centre + rate_s[z] * (flux + pow_s[z]), flow_z

    def first_step(z, flow_below):
        temp2[z], flow_z = heat(z, flow_below, temp, True)
        return flow_z

    blank = mod[0]
    lax.fori_loop(0, layers, first_step, cond[layers], unroll=4)

    def second_step(z, flow_below):
        value, flow_z = heat(z, flow_below, temp2, False)
        warmed[z] = value[HALO : HALO + rows, 0:cols]
        strain[z + 1] = strain[z + 1] * value[kept]
        return flow_z

    lax.fori_loop(0, layers, second_step, cond[layers], unroll=4)
    results = [pltpu.make_async_copy(warmed, warmed_out, out_sem.at[0])]
    results[0].start()


    def matrix_planes(p):
        f = mod[p]
        sx, sy, sxsy, ex, ey, cross = matrix_parts(f)
        z0, z1 = diag_z(f, sx, sy, sxsy)
        x0, x1 = diag_x(f, sx, sy, sxsy)
        y0, y1 = diag_y(f, sx, sy, sxsy)
        zero = jnp.zeros_like(f)
        return (
            (z0, x0, y0, zero, zero, 0.125 * cross),
            (z1, x1, y1, zero, zero, (1.0 / 18.0) * cross),
            (zero, zero, zero, ex, ey, zero),
        )

    def matrix_emit(p, out, extra):
        diagonal = (ANCHOR + K_TOTAL) * mod[p] - 1.0
        for c in range(6):
            mats[c, p] = out[c] + diagonal if c < 3 else out[c]
        return extra

    stream(layers, 6, blank, matrix_planes, matrix_emit, 0)

    def fold(inner):
        result = inner[0:8]
        for r in range(8, rows, 8):
            result = result + inner[r : r + 8]
        return result

    tile = mod[0, 0:8, 0:cols]

    def load_planes(p):
        m, s = mod[p], strain[p]
        parts = [gradient_stencil(f) for f in (s, m, m * s)]
        return tuple(tuple(a for part in parts for a in part[i]) for i in range(3))

    def load_emit(p, out, acc):
        m, s, inside = mod[p], strain[p], mask[p]
        for c in range(3):
            value = -inside * (m * out[c] + s * out[3 + c] + out[6 + c])
            v[0, c, p] = value
            inner = value[inner_rows, 0:cols]
            vown[0, c, p] = inner
            acc = acc + fold(inner * inner)
        return acc

    moment_s[0] = stream(layers, 9, blank, load_planes, load_emit, tile)

    def shares(k):
        found = []
        for step in range(1, nz):
            there = lax.rem(iz + step, nz)
            found.append(
                pltpu.make_async_remote_copy(
                    src_ref=vown.at[k, :, pl.ds(1 + there * share, share)],
                    dst_ref=vrecv.at[k, step - 1],
                    send_sem=vsend_sem.at[k, step - 1], recv_sem=vrecv_sem.at[k, step - 1],
                    device_id=(ix, iy, there), device_id_type=MESH,
                )
            )
        return found

    def share_basis(k):
        for copy in shares(k):
            copy.start()

    share_basis(0)

    def apply(k, width):
        def planes(p):
            m = mod[p]
            u = [v[k, c, p] for c in range(3)]
            first = vector_stencil(*u, width)
            second = vector_stencil(*[m * f for f in u], width)
            return tuple(a + b for a, b in zip(first, second))

        def emit(p, out, acc):
            m = mod[p, :, 0:width]
            u = [v[k, c, p, :, 0:width] for c in range(3)]
            zz, xx, yy, zx, zy, xy = [mats[c, p, :, 0:width] for c in range(6)]
            grown = (
                zz * u[0] + zx * u[1] + zy * u[2],
                zx * u[0] + xx * u[1] + xy * u[2],
                zy * u[0] + xy * u[1] + yy * u[2],
            )
            odd, even = acc
            for c in range(3):
                value = grown[c] - m * out[c] - out[3 + c]
                if width > cols:
                    value = mask[p] * value
                    v[k + 1, c, p] = value
                inner = value[inner_rows, 0:cols]
                vown[k + 1, c, p] = inner
                odd = odd + fold(inner * vown[k, c, p])
                even = even + fold(inner * inner)
            return odd, even

        odd, even = stream(layers, 6, mod[0, :, 0:width], planes, emit, (tile, tile))
        moment_s[2 * k + 1] = odd
        moment_s[2 * k + 2] = even

    def grow(k, _):
        apply(k, 2 * cols)
        share_basis(k + 1)
        return 0

    lax.fori_loop(0, ITERS - 1, grow, 0)
    apply(ITERS - 1, cols)

    lane8 = lax.broadcasted_iota(jnp.int32, (1, cols), 1)
    row = jnp.zeros((1, cols), jnp.float32)
    for k in range(2 * ITERS):
        line = jnp.sum(moment_s[k], axis=0, keepdims=True)
        row = jnp.where(lane8 == k, jnp.sum(line, axis=1, keepdims=True), row)
    red_src[...] = row
    red_buf[me] = row

    def spread(k):
        there = lax.rem(me + k, total)
        return pltpu.make_async_remote_copy(
            src_ref=red_src, dst_ref=red_buf.at[me], send_sem=rsend_sem.at[k],
            recv_sem=rrecv_sem.at[k], device_id=coords(there), device_id_type=MESH,
        )

    def collect(k):
        there = lax.rem(me + total - k, total)
        return pltpu.make_async_remote_copy(
            src_ref=red_src, dst_ref=red_buf.at[there], send_sem=rsend_sem.at[k],
            recv_sem=rrecv_sem.at[k], device_id=coords(there), device_id_type=MESH,
        )

    def start(k, _):
        spread(k).start()
        return 0

    def finish(k, _):
        collect(k).wait_recv()
        return 0

    def sent(k, _):
        spread(k).wait_send()
        return 0

    lax.fori_loop(1, total, start, 0, unroll=4)
    share_basis(ITERS)
    lax.fori_loop(1, total, finish, 0, unroll=4)

    def add(k, acc):
        return acc + red_buf[k]

    summed = lax.fori_loop(0, total, add, jnp.zeros((1, cols), jnp.float32), unroll=4)
    m = [
        jnp.sum(jnp.where(lane8 == k, summed, 0.0), axis=1, keepdims=True) for k in range(2 * ITERS)
    ]

    def inner(a, b):
        value = None
        for i, x in enumerate(a):
            for j, y in enumerate(b):
                if x is not None and y is not None:
                    term = x * y * m[i + j]
                    value = term if value is None else value + term
        return value

    def plus(a, factor, b):
        out = []
        for x, y in zip(a, b):
            if y is None:
                out.append(x)
            else:
                out.append(factor * y if x is None else x + factor * y)
        return out

    one = jnp.ones((1, 1), jnp.float32)
    size = ITERS + 1
    res = [one] + [None] * ITERS
    dire = list(res)
    sol = [None] * size
    rr = m[0]
    for number in range(ITERS):
        image = plus(list(dire), 1.0, [None] + dire[:-1])
        alpha = rr / inner(dire, image)
        sol = plus(sol, alpha, dire)
        res = plus(res, -alpha, image)
        if number + 1 < ITERS:
            new = inner(res, res)
            dire = plus(res, new / rr, dire)
            rr = new
    res = [shift_scalar * x for x in res]

    for step in range(nz):
        where = pl.ds(pl.multiple_of(lax.rem(iz + nz - step, nz) * cols, cols), cols)
        for index, (weights, held, target) in enumerate(
            ((sol[:ITERS], solution, solution_out), (res, residual, residual_out))
        ):
            if step:
                for k in range(ITERS) if index == 0 else (ITERS,):
                    shares(k)[step - 1].wait_recv()

            def combine(z, _, step=step, weights=weights, held=held):
                for c in range(3):
                    value = None
                    for k, weight in enumerate(weights):
                        part = vown[k, c, 1 + iz * share + z] if step == 0 else vrecv[k, step - 1, c, z]
                        value = weight * part if value is None else value + weight * part
                    held[step, c, z] = value
                return 0

            lax.fori_loop(0, share, combine, 0, unroll=4)
            results.append(
                pltpu.make_async_copy(
                    held.at[step], target.at[:, :, :, where], out_sem.at[1 + 2 * step + index]
                )
            )
            results[-1].start()

    for target, _, copies, _, _ in moves:
        @pl.when(target)
        def _(copies=copies):
            for copy in copies:
                copy.wait_send()
    for k in range(ITERS + 1):
        for copy in shares(k):
            copy.wait_send()
    lax.fori_loop(1, total, sent, 0)
    for copy in results:
        copy.wait()


def per_device(sizes, *arrays):
    nx, ny, nz = sizes
    layers, rows, cols = arrays[0].shape
    total = nx * ny * nz
    share = layers // nz
    ext = (rows + 2 * HALO, 2 * cols)
    f32, i32 = jnp.float32, jnp.int32
    vmem = pltpu.VMEM
    dma = pltpu.SemaphoreType.DMA
    out = jax.ShapeDtypeStruct((3, share, rows, cols * nz), f32)
    plane = vmem((layers, *ext), f32)
    kept = (rows + 2 * EDGE, 2 * cols)
    padded = vmem((layers + 2, *kept), f32)
    half = vmem((nz, 3, share, rows, cols), f32)
    return pl.pallas_call(
        functools.partial(kernel, sizes),
        out_shape=(jax.ShapeDtypeStruct((layers, rows, cols), f32), out, out),
        in_specs=[pl.BlockSpec(memory_space=pltpu.HBM)] * 5,
        out_specs=[pl.BlockSpec(memory_space=pl.ANY)] * 3,
        scratch_shapes=[
            pltpu.SMEM(arrays[3].shape, f32), pltpu.SMEM(arrays[4].shape, f32), dma((2,)),
            vmem((layers, rows, cols), f32), half, half,
            vmem((ITERS + 1, 3, layers + 1, rows, cols), f32),
            vmem((2 * ITERS + 1, 8, cols), f32), dma((1 + 2 * nz,)),
            plane, plane, vmem((layers, *ext), i32), vmem((layers, *ext), i32),
            vmem((layers + 1, *ext), f32), padded, padded, padded,
            plane, plane, plane, plane, plane,
            vmem((6, layers + 1, *kept), f32),
            vmem((ITERS, 3, layers + 2, *kept), f32),
            vmem((ITERS + 1, nz - 1, 3, share, rows, cols), f32),
            vmem((2, rows, cols), f32), vmem((2, 2, rows, cols), i32),
            vmem((2, ext[0], cols), f32), vmem((2, 2, ext[0], cols), i32),
            vmem((1, cols), f32), vmem((total, 1, cols), f32),
            dma((3,)), dma((8, 3)), dma((8, 3)),
            dma((ITERS + 1, nz - 1)), dma((ITERS + 1, nz - 1)), dma((total,)), dma((total,)),
        ],
        compiler_params=pltpu.CompilerParams(
            collective_id=0, has_side_effects=True, vmem_limit_bytes=40 * 1024 * 1024
        ),
    )(*[pltpu.with_memory_space_constraint(a, pltpu.HBM) for a in arrays])


def solution(mesh):
    sizes = tuple(mesh.shape[axis] for axis in ("gx", "gy", "gz"))
    split = P(None, "gx", ("gy", "gz"))
    out = P(None, "gz", "gx", "gy")
    return jax.shard_map(
        functools.partial(per_device, sizes),
        mesh=mesh,
        in_specs=(split, split, split, P(), P()),
        out_specs=(split, out, out),
        check_vma=False,
    )
```
